16 devices in a mesh: fsdp: 16 (over z, y, x, core).
Axes of the slice: x: 2, y: 2, z: 2, core: 2. Of those that a mesh axis runs over, the one named last changes fastest.
Arguments:
- x_saved: bfloat16 [2, 2, 16, 1024, 1024], P(None, None, 'fsdp')
- grad_out: bfloat16 [2, 16, 1024, 1024], P(None, 'fsdp')
- x_next: bfloat16 [2, 16, 1024, 1024], P(None, 'fsdp')
- w_up: bfloat16 [2, 2, 1024, 4096], replicated
- w_down: bfloat16 [2, 2, 4096, 1024], replicated
- acc_up: float32 [2, 2, 1024, 4096], P(None, None, 'fsdp')
- acc_down: float32 [2, 2, 4096, 1024], P(None, None, 'fsdp')
- master_up: float32 [2, 2, 1024, 4096], P(None, None, 'fsdp')
- master_down: float32 [2, 2, 4096, 1024], P(None, None, 'fsdp')
- moment1_up: float32 [2, 2, 1024, 4096], P(None, None, 'fsdp')
- moment1_down: float32 [2, 2, 4096, 1024], P(None, None, 'fsdp')
- moment2_up: float32 [2, 2, 1024, 4096], P(None, None, 'fsdp')
- moment2_down: float32 [2, 2, 4096, 1024], P(None, None, 'fsdp')
Outputs:
- output 1: float32 [2, 2, 1024, 4096], P(None, None, 'fsdp')
- output 2: float32 [2, 2, 4096, 1024], P(None, None, 'fsdp')
- output 3: float32 [2, 2, 1024, 4096], P(None, None, 'fsdp')
- output 4: float32 [2, 2, 4096, 1024], P(None, None, 'fsdp')
- output 5: float32 [2, 2, 1024, 4096], P(None, None, 'fsdp')
- output 6: float32 [2, 2, 4096, 1024], P(None, None, 'fsdp')
- output 7: bfloat16 [2, 16, 1024, 1024], P(None, 'fsdp')
All inputs are finite; a program needn't handle non-finite values.
Results may differ from the reference program's by a relative error of at most 0.00724236.
Values are sent between devices in bfloat16 or wider.
A program may use at most 1 GiB of HBM per device.

```python
import functools
import jax
import jax.numpy as jnp
from jax import lax

D = 1024
FF = 4096
BATCH = 16
SEQ_LEN = 1024
GROUPS = 16
STAGES = 2
LAYERS = 2
MICROBATCHES = 2
ADAM_STEP = 2
TOKENS = BATCH // GROUPS * SEQ_LEN
LEARN_RATE = 0.005
BETA_ONE = 0.9
BETA_TWO = 0.95
ADAM_EPS = 1e-8
WEIGHT_DECAY = 0.1


def setup_inputs(seed: int = 0) -> dict:
    key_list = jax.random.split(jax.random.key(seed), 13)
    row_count = BATCH * SEQ_LEN
    scale_up = 0.3 * row_count ** 0.5
    scale_down = 0.7 * row_count ** 0.5
    tok_shape = (STAGES, BATCH, SEQ_LEN, D)
    up_shape = (STAGES, LAYERS, D, FF)
    down_shape = (STAGES, LAYERS, FF, D)
    x_saved = jax.random.normal(key_list[0], (STAGES, LAYERS, BATCH, SEQ_LEN, D), jnp.float32).astype(jnp.bfloat16)
    grad_out = jax.random.normal(key_list[1], tok_shape, jnp.float32).astype(jnp.bfloat16)
    x_next = jax.random.normal(key_list[2], tok_shape, jnp.float32).astype(jnp.bfloat16)
    w_up = (jax.random.normal(key_list[3], up_shape, jnp.float32) * D ** -0.5).astype(jnp.bfloat16)
    w_down = (jax.random.normal(key_list[4], down_shape, jnp.float32) * FF ** -0.5).astype(jnp.bfloat16)
    acc_up = jax.random.normal(key_list[5], up_shape, jnp.float32) * scale_up
    acc_down = jax.random.normal(key_list[6], down_shape, jnp.float32) * scale_down
    master_up = jax.random.normal(key_list[7], up_shape, jnp.float32) * D ** -0.5
    master_down = jax.random.normal(key_list[8], down_shape, jnp.float32) * FF ** -0.5
    moment1_up = jax.random.normal(key_list[9], up_shape, jnp.float32) * (0.05 * scale_up)
    moment1_down = jax.random.normal(key_list[10], down_shape, jnp.float32) * (0.05 * scale_down)
    moment2_up = jax.random.uniform(key_list[11], up_shape, jnp.float32, 0.02, 0.06) * scale_up ** 2
    moment2_down = jax.random.uniform(key_list[12], down_shape, jnp.float32, 0.02, 0.06) * scale_down ** 2
    return {'x_saved': x_saved, 'grad_out': grad_out, 'x_next': x_next, 'w_up': w_up, 'w_down': w_down, 'acc_up': acc_up, 'acc_down': acc_down, 'master_up': master_up, 'master_down': master_down, 'moment1_up': moment1_up, 'moment1_down': moment1_down, 'moment2_up': moment2_up, 'moment2_down': moment2_down}


def backward_layer(x_in, cotangent, w_one, w_two):
    hidden = jnp.dot(x_in, w_one, preferred_element_type=jnp.float32)
    gelu_out, gelu_vjp = jax.vjp(jax.nn.gelu, hidden)
    gelu_out = gelu_out.astype(jnp.bfloat16)
    grad_act = jnp.dot(cotangent, w_two.T, preferred_element_type=jnp.float32)
    grad_hidden = gelu_vjp(grad_act)[0].astype(jnp.bfloat16)
    part_down = jnp.dot(gelu_out.T, cotangent, preferred_element_type=jnp.float32)
    part_up = jnp.dot(x_in.T, grad_hidden, preferred_element_type=jnp.float32)
    return part_up, part_down, grad_hidden


def stage_grads(x_layers, grad_top, up_stack, down_stack):
    x_blocks = jnp.swapaxes(x_layers.reshape(LAYERS, GROUPS, TOKENS, D), 0, 1)
    grad_blocks = grad_top.reshape(GROUPS, TOKENS, D)

    def scan_body(carry, block_pair):
        sum_up, sum_down = carry
        x_block, cotangent = block_pair
        up_parts = [None] * LAYERS
        down_parts = [None] * LAYERS
        for layer_id in reversed(range(LAYERS)):
            part_up, part_down, grad_hidden = backward_layer(x_block[layer_id], cotangent, up_stack[layer_id], down_stack[layer_id])
            up_parts[layer_id] = part_up
            down_parts[layer_id] = part_down
            if layer_id > 0:
                cotangent = (cotangent.astype(jnp.float32) + jnp.dot(grad_hidden, up_stack[layer_id].T, preferred_element_type=jnp.float32)).astype(jnp.bfloat16)
        return (sum_up + jnp.stack(up_parts), sum_down + jnp.stack(down_parts)), None

    start_sums = (jnp.zeros((LAYERS, D, FF), jnp.float32), jnp.zeros((LAYERS, FF, D), jnp.float32))
    final_sums, scan_rest = lax.scan(scan_body, start_sums, (x_blocks, grad_blocks))
    return final_sums


def adam_update(acc_part, grad_new, master, moment_one, moment_two):
    grad_mean = (acc_part + grad_new) / MICROBATCHES
    moment_one = BETA_ONE * moment_one + (1.0 - BETA_ONE) * grad_mean
    moment_two = BETA_TWO * moment_two + (1.0 - BETA_TWO) * grad_mean * grad_mean
    corr_one = 1.0 - BETA_ONE ** ADAM_STEP
    corr_two = 1.0 - BETA_TWO ** ADAM_STEP
    step_dir = (moment_one / corr_one) / (jnp.sqrt(moment_two / corr_two) + ADAM_EPS)
    master = master - LEARN_RATE * (step_dir + WEIGHT_DECAY * master)
    return master, moment_one, moment_two


def forward_rows(x_rows, up_stack, down_stack):
    for layer_id in range(LAYERS):
        hidden = jnp.dot(x_rows, up_stack[layer_id], preferred_element_type=jnp.float32)
        gelu_out = jax.nn.gelu(hidden).astype(jnp.bfloat16)
        mlp_val = jnp.dot(gelu_out, down_stack[layer_id], preferred_element_type=jnp.float32)
        x_rows = (x_rows.astype(jnp.float32) + mlp_val).astype(jnp.bfloat16)
    return x_rows


def reference(x_saved, grad_out, x_next, w_up, w_down, acc_up, acc_down, master_up, master_down, moment1_up, moment1_down, moment2_up, moment2_down):
    grads_up = []
    grads_down = []
    for stage_id in range(STAGES):
        sum_up, sum_down = stage_grads(x_saved[stage_id], grad_out[stage_id], w_up[stage_id], w_down[stage_id])
        grads_up.append(sum_up)
        grads_down.append(sum_down)
    new_master_up, new_moment1_up, new_moment2_up = adam_update(acc_up, jnp.stack(grads_up), master_up, moment1_up, moment2_up)
    new_master_down, new_moment1_down, new_moment2_down = adam_update(acc_down, jnp.stack(grads_down), master_down, moment1_down, moment2_down)
    new_up = new_master_up.astype(jnp.bfloat16)
    new_down = new_master_down.astype(jnp.bfloat16)
    outs_next = []
    for stage_id in range(STAGES):
        row_blocks = x_next[stage_id].reshape(GROUPS, TOKENS, D)
        moved = lax.map(functools.partial(forward_rows, up_stack=new_up[stage_id], down_stack=new_down[stage_id]), row_blocks)
        outs_next.append(moved.reshape(BATCH, SEQ_LEN, D))
    y_next = jnp.stack(outs_next)
    return (new_master_up, new_master_down, new_moment1_up, new_moment1_down, new_moment2_up, new_moment2_down, y_next)
```

```python
import jax
import jax.numpy as jnp
from jax import lax
from jax.sharding import Mesh, PartitionSpec as P

LEARN_RATE = 0.005
BETA_ONE = 0.9
BETA_TWO = 0.95
ADAM_EPS = 1e-8
WEIGHT_DECAY = 0.1
MICROBATCHES = 2
ADAM_STEP = 2
CORES = 2
SWAP = [(0, 1), (1, 0)]
F32 = jnp.float32
BF16 = jnp.bfloat16


def adam_update(acc_part, grad_new, master, moment_one, moment_two):
    grad_mean = (acc_part + grad_new) / MICROBATCHES
    moment_one = BETA_ONE * moment_one + (1.0 - BETA_ONE) * grad_mean
    moment_two = BETA_TWO * moment_two + (1.0 - BETA_TWO) * grad_mean * grad_mean
    corr_one = 1.0 - BETA_ONE ** ADAM_STEP
    corr_two = 1.0 - BETA_TWO ** ADAM_STEP
    step_dir = (moment_one / corr_one) / (jnp.sqrt(moment_two / corr_two) + ADAM_EPS)
    master = master - LEARN_RATE * (step_dir + WEIGHT_DECAY * master)
    return master, moment_one, moment_two


def swap(val):
    return lax.ppermute(val, 'core', SWAP)


def dot(a, b, ca, cb):
    return lax.dot_general(a, b, (((ca,), (cb,)), ((), ())), preferred_element_type=F32)


def pair(own):
    return jnp.concatenate([own, swap(own)], axis=0)


def scatter_sum(part, chips):
    part = part.astype(BF16).reshape((chips, -1) + part.shape[1:])
    received = lax.all_to_all(part, 'chip', 0, 0, tiled=True)
    return jnp.sum(received, axis=0, dtype=F32)


def solution(mesh):
    chips = mesh.shape['fsdp'] // CORES
    mesh2 = Mesh(mesh.devices.reshape(chips, CORES), ('chip', 'core'))
    both = ('chip', 'core')
    tok_spec = P(None, both)
    layer_spec = P(None, None, both)
    rep_spec = P()

    def device_step(x_saved, grad_out, x_next, w_up, w_down, acc_up, acc_down, master_up, master_down, moment1_up, moment1_down, moment2_up, moment2_down):
        stages, layers = x_saved.shape[:2]
        tokens, width = x_saved.shape[-2:]
        ff = w_up.shape[-1]
        half = ff // CORES
        blk = ff // (chips * CORES)
        core = lax.axis_index('core')

        def split_cols(w, which):
            return lax.dynamic_index_in_dim(w.reshape(w.shape[0], chips, CORES, blk), which, 2, keepdims=False).reshape(w.shape[0], half)

        def join_cols(low, high):
            rows = low.shape[0]
            return jnp.stack([low.reshape(rows, chips, blk), high.reshape(rows, chips, blk)], axis=2).reshape(rows, ff)

        state = [[[None] * layers for s in range(stages)] for i in range(6)]
        full_up = [[None] * layers for s in range(stages)]
        full_down = [[None] * layers for s in range(stages)]
        y_list = []
        for s in range(stages):
            own_cot = grad_out[s, 0]
            cot = pair(own_cot)
            for l in reversed(range(layers)):
                x = pair(x_saved[s, l, 0])
                w1 = split_cols(w_up[s, l], core)
                w2 = lax.dynamic_index_in_dim(w_down[s, l].reshape(chips, CORES, blk, width), core, 1, keepdims=False).reshape(half, width)
                hidden = dot(x, w1, 1, 0)
                gelu_out, gelu_vjp = jax.vjp(jax.nn.gelu, hidden)
                gelu_out = gelu_out.astype(BF16)
                part_down = dot(gelu_out, cot, 0, 0)
                sum_down = scatter_sum(part_down, chips)
                grad_act = dot(cot, w2, 1, 1)
                grad_hidden = gelu_vjp(grad_act)[0].astype(BF16)
                if l > 0:
                    back = dot(grad_hidden, w1, 1, 1)
                    own_cot = (own_cot.astype(F32) + back[:tokens] + swap(back[tokens:])).astype(BF16)
                    cot = pair(own_cot)
                part_up = dot(x, grad_hidden, 0, 0)
                sum_up = scatter_sum(part_up, chips)
                rows = sum_up.shape[0] // CORES
                mine = lax.dynamic_slice_in_dim(sum_up, core * rows, rows, 0)
                other = swap(lax.dynamic_slice_in_dim(sum_up, (1 - core) * rows, rows, 0))
                low = jnp.where(core == 0, mine, other)
                high = jnp.where(core == 0, other, mine)
                sum_up = join_cols(low, high)
                new_down = adam_update(acc_down[s, l], sum_down, master_down[s, l], moment1_down[s, l], moment2_down[s, l])
                new_up = adam_update(acc_up[s, l], sum_up, master_up[s, l], moment1_up[s, l], moment2_up[s, l])
                for i in range(3):
                    state[2 * i][s][l] = new_up[i]
                    state[2 * i + 1][s][l] = new_down[i]
                full_down[s][l] = lax.all_gather(new_down[0].astype(BF16), 'chip', axis=0, tiled=True)
                bf_up = new_up[0].astype(BF16)
                mine = split_cols(bf_up, core)
                other = swap(split_cols(bf_up, 1 - core))
                low = jnp.where(core == 0, mine, other)
                high = jnp.where(core == 0, other, mine)
                full_up[s][l] = lax.all_gather(jnp.concatenate([low, high], axis=0), 'chip', axis=0, tiled=True)
            own_x = x_next[s, 0]
            for l in range(layers):
                x = pair(own_x)
                hidden = dot(x, full_up[s][l], 1, 0)
                gelu_out = jax.nn.gelu(hidden).astype(BF16)
                mlp = dot(gelu_out, full_down[s][l], 1, 0)
                own_x = (own_x.astype(F32) + (mlp[:tokens] + swap(mlp[tokens:]))).astype(BF16)
            y_list.append(own_x)
        outs = tuple(jnp.stack([jnp.stack(per) for per in entry]) for entry in state)
        return outs + (jnp.stack(y_list)[:, None],)

    return jax.shard_map(device_step, mesh=mesh2, in_specs=(layer_spec, tok_spec, tok_spec, rep_spec, rep_spec) + (layer_spec,) * 8, out_specs=(layer_spec,) * 6 + (tok_spec,), check_vma=False)
```

```python
import jax
import jax.numpy as jnp
from jax import lax
from jax.experimental import pallas as pl
from jax.experimental.pallas import tpu as pltpu
from jax.sharding import PartitionSpec as P

LEARN_RATE = 0.005
BETA_ONE = 0.9
BETA_TWO = 0.95
ADAM_EPS = 1e-8
WEIGHT_DECAY = 0.1
MICROBATCHES = 2
ADAM_STEP = 2
F32 = jnp.float32
BF16 = jnp.bfloat16
MESH = pl.DeviceIdType.MESH
GELU_C = 0.7978845608028654
GELU_K = 0.044715
AXES = 'zyx'
ORDERS = ('xyz', 'yzx', 'zxy')
COLS = {'d': ((0, 384), (384, 384), (768, 256)), 'u': ((0, 640), (640, 640), (1280, 768))}
ROWS = {'d': 256, 'u': 128}
WIDE = {'d': 1024, 'u': 2048}
T = 1024
D = 1024
H = 2048
TM = 256
TF = 512
PAIR = (0, 1)
QUADS = 4
SEMS = 230
CHIPS = 8
SUB = 16
STEPS = {'d': (1, 2, 3, 6, 7), 'u': (1, 2, 3, 4, 5, 6, 7)}
MATS = {'A': (0, 1, 'd'), 'B': (0, 1, 'u'), 'C': (0, 0, 'd'), 'D': (0, 0, 'u'), 'E': (1, 1, 'd'), 'F': (1, 1, 'u'), 'G': (1, 0, 'd'), 'H': (1, 0, 'u')}
ORDER = ('jjjjjjAjjjAjBjjjjABCjjDAjjCjEjDjjCDjFDjDBHFCEDHFBD', 'FGHBCHHFBGjjHjBAjGjjFEGHjjGjEjFjjjjEjjjjjj',)

def adam_update(acc_part, grad_new, master, moment_one, moment_two):
    grad_mean = (acc_part + grad_new) / MICROBATCHES
    moment_one = BETA_ONE * moment_one + (1.0 - BETA_ONE) * grad_mean
    moment_two = BETA_TWO * moment_two + (1.0 - BETA_TWO) * grad_mean * grad_mean
    corr_one = 1.0 - BETA_ONE ** ADAM_STEP
    corr_two = 1.0 - BETA_TWO ** ADAM_STEP
    step_dir = (moment_one / corr_one) / (jnp.sqrt(moment_two / corr_two) + ADAM_EPS)
    master = master - LEARN_RATE * (step_dir + WEIGHT_DECAY * master)
    return master, moment_one, moment_two


def jobs_of():
    for s in PAIR:
        for l in reversed(PAIR):
            for g in range(QUADS // (1 if (s, l) == (0, 1) else 2)):
                yield 'k', s, l, g
            if l:
                yield 'bk', s, l, 1
                yield 'bk', s, l, 0
            yield 'j3', s, l, 0
            if l:
                yield 'cb', s, l, 0
            yield 'j3', s, l, 1
    for s in PAIR:
        for l in PAIR:
            for name, half in (('f1', 1 - l), ('f1', l), ('f2', 1), ('f2', 0), ('cf', 0)):
                yield name, s, l, half


def gelu_parts(h):
    sq = h * h
    th = jnp.tanh(GELU_C * (h + GELU_K * (h * sq)))
    return sq, th


def dot(a, b, ca, cb):
    return lax.dot_general(a, b, (((ca,), (cb,)), ((), ())), preferred_element_type=F32)


def step_kernel(*refs):
    it = iter(refs)
    take = lambda n: [next(it) for i in range(n)]
    x_saved, grad_out, x_next, w_up, w_down = take(5)
    acc, mast, mom1, mom2 = [dict(zip('ud', take(2))) for i in range(4)]
    nmast, nmom1, nmom2 = [dict(zip('ud', take(2))) for i in range(3)]
    (y_out,) = take(1)
    xr, tokr, pr = take(3)
    part, r1, r2o, r2f, r3, aw = [dict(zip('du', take(2))) for i in range(6)]
    gd, go, gx, ws = take(4)
    xv, yv, w1v, w2v, av, hv, fst, dwd, dwu = take(9)
    sb, so, r3v = [dict(zip('du', take(2))) for i in range(3)]
    ssem, rsem, w1sem, w2sem, xsem, ysem, dwsem, sbsem, msem = take(9)

    me = lax.axis_index('fsdp')
    pos = {'z': lax.div(me, 8), 'y': lax.rem(lax.div(me, 4), 2), 'x': lax.rem(lax.div(me, 2), 2)}
    core = lax.rem(me, 2)
    flip = {a: 1 - pos[a] for a in AXES}
    peer = {a: me + step * (1 - 2 * pos[a]) for a, step in (('z', 8), ('y', 4), ('x', 2))}
    peer['core'] = me + 1 - 2 * core
    spot = tuple(pos[a] for a in AXES)

    sem_ids = {}
    sends = {}

    def remote(key, src, dst, axis):
        n = sem_ids.setdefault(key, len(sem_ids))
        cp = pltpu.make_async_remote_copy(src_ref=src, dst_ref=dst, send_sem=ssem.at[n], recv_sem=rsem.at[n], device_id=(peer[axis],), device_id_type=MESH)
        cp.start()
        sends[key] = cp

    recv = lambda key: sends[key].wait_recv()
    unsent = set()

    def wait_send(key):
        if key in sends and key not in unsent:
            unsent.add(key)
            sends[key].wait_send()

    def cut(ref, i, fix, c0, n):
        return ref.at[(i,) + tuple(fix.get(a, slice(None)) for a in AXES) + (slice(None), pl.ds(c0, n))]

    def local(src, dst, sem):
        cp = pltpu.make_async_copy(src, dst, sem)
        cp.start()
        return cp

    loads = {'w1': [], 'w2': [], 'xa': [], 'xb': [], 'ya': [], 'yb': []}

    def ready(*names):
        for name in names:
            for cp in loads[name]:
                cp.wait()
            loads[name] = []

    def load_w1(s, l):
        loads['w1'] = [local(w_up.at[s, l, :, pl.ds(512 * c + 256 * core, 256)], w1v.at[:, pl.ds(256 * c, 256)], w1sem.at[c]) for c in range(8)]

    def load_w2(s, l):
        loads['w2'] = [local(w_down.at[s, l, c, core], w2v.at[pl.ds(256 * c, 256)], w2sem.at[c]) for c in range(8)]

    def load_new(kind, i):
        dst, sem, name, rows = (w1v, w1sem, 'w1', 128) if kind == 'u' else (w2v, w2sem, 'w2', 256)
        loads[name] = [local(aw[kind].at[i, c // 4, (c // 2) % 2, c % 2], dst.at[pl.ds(rows * c, rows)], sem.at[c]) for c in range(8)]

    def load_x(half, src):
        loads[('xa', 'xb')[half]] = [local(src, xv.at[pl.ds(T * half, T)], xsem.at[half])]

    def load_y(half, src):
        loads[('ya', 'yb')[half]] = [local(src, yv.at[pl.ds(T * half, T)], ysem.at[half])]

    def slab(n, size):
        return pl.ds(pl.multiple_of(n * size, size), size)

    def quad(g):
        return lax.rem(pos['z'] + 1 + lax.div(g, 2), 2), lax.rem(pos['y'] + 1 + lax.rem(g, 2), 2)

    def backward(i, g0, count, hook=None):
        def block(g, hook=None):
            zz, yy = quad(g)
            fs = slab(2 * zz + yy, TF)

            def body(n, carry):
                ts = slab(n, TM)
                h = dot(xv[ts, :], w1v[:, fs], 1, 0)
                da = dot(yv[ts, :], w2v[fs, :], 1, 1)
                sq, th = gelu_parts(h)
                cdf = 0.5 * (1.0 + th)
                av[ts, fs] = (h * cdf).astype(BF16)
                slope = cdf + 0.5 * h * (1.0 - th * th) * (GELU_C * (1.0 + 3.0 * GELU_K * sq))
                hv[ts, fs] = (da * slope).astype(BF16)
                return carry
            tiles = T // TM
            if hook is not None:
                lax.fori_loop(0, tiles, body, 0)
                hook()
                lax.fori_loop(tiles, 2 * tiles, body, 0)
            else:
                lax.fori_loop(0, 2 * tiles, body, 0)

            def out(n):
                return pltpu.make_async_copy(dwd.at[n], part['d'].at[i, zz, yy, n], dwsem.at[n])

            def body2(n, carry):
                f0 = slab(2 * (2 * zz + yy) + n, TM)

                def inner(c, carry):
                    cs = slab(c, TF)
                    dwd[n, :, cs] = dot(av[:, f0], yv[:, cs], 0, 0).astype(BF16)
                    return carry
                lax.fori_loop(0, D // TF, inner, 0)
                out(n).start()
                return carry
            lax.fori_loop(0, 2, body2, 0)
            for n in PAIR:
                out(n).wait()
        if count == 1:
            block(jnp.int32(g0), hook)
        else:
            def each(g, carry):
                block(g)
                return carry
            lax.fori_loop(g0, g0 + count, each, 0)

    def j3(i, half):
        def out(n):
            return pltpu.make_async_copy(dwu.at[n], part['u'].at[i, half, n], dwsem.at[n])

        def body(n, carry):
            def inner(c, carry):
                fs = slab(c, TF)
                res = dot(xv[:, slab(2 * half + n, TM)], hv[:, fs], 0, 0).astype(BF16)
                for e in PAIR:
                    dwu[n, e, :, fs] = res[128 * e:128 * e + 128]
                return carry
            lax.fori_loop(0, H // TF, inner, 0)
            out(n).start()
            return carry
        lax.fori_loop(0, 2, body, 0)
        for n in PAIR:
            out(n).wait()

    def proj(half, src, dst, w, cb, send=None):
        def body(n, carry):
            def inner(c, carry):
                cs = slab(c, TF)
                wt = w[cs, :] if cb else w[:, cs]
                fst[dst, slab(n, TM), cs] = dot(src[slab(T // TM * half + n, TM), :], wt, 1, cb)
                return carry
            return lax.fori_loop(0, D // TF, inner, carry)
        if send is None:
            lax.fori_loop(0, T // TM, body, 0)
            return
        for e in PAIR:
            lax.fori_loop(2 * e, 2 * e + 2, body, 0)
            rows = pl.ds(TF * e, TF)
            remote(('pr', send, e), fst.at[0, rows], pr.at[send, rows], 'core')

    def f1(half):
        def body(n, carry):
            ts = slab(T // TM * half + lax.div(n, H // TF), TM)
            fs = slab(lax.rem(n, H // TF), TF)
            h = dot(xv[ts, :], w1v[:, fs], 1, 0)
            sq, th = gelu_parts(h)
            av[ts, fs] = (h * (0.5 * (1.0 + th))).astype(BF16)
            return carry
        lax.fori_loop(0, (T // TM) * (H // TF), body, 0)

    def combine(n_pr, base):
        cps = []
        for e in PAIR:
            recv(('pr', n_pr, e))
            wait_send(('pr', n_pr, e))
            rows = pl.ds(TF * e, TF)
            cps.append(local(pr.at[n_pr, rows], fst.at[0, rows], msem.at[2 * e]))
        for e in PAIR:
            cps[e].wait()

            def body(n, carry):
                rows = slab(n, SUB)
                base[rows, :] = (base[rows, :].astype(F32) + (fst[1, rows, :] + fst[0, rows, :])).astype(BF16)
                return carry
            lax.fori_loop(TF * e // SUB, TF * (e + 1) // SUB, body, 0)

    def streams(kind):
        return zip(range(3), COLS[kind], ORDERS)

    last_so = {'d': None, 'u': None}
    last_gx = [None]
    first = {}

    def fetch(kind, items):
        cps = [local(src, dst, sbsem.at[n]) for n, (src, dst) in enumerate(items)]
        for cp in cps:
            cp.wait()

    def send_own(kind, m):
        i = 2 * m[0] + m[1]
        for q, (c0, n), (a, b, c) in streams(kind):
            fix = {a: pos[a], b: flip[b]}
            remote(('r2o', m, q), cut(part[kind], i, fix, c0, n), cut(r2o[kind], i, fix, c0, n), b)

    def send_half(kind, m, fix, which=AXES):
        i = 2 * m[0] + m[1]
        for q, (c0, n), (a, b, c) in streams(kind):
            if a in which:
                where = {**fix, a: flip[a]}
                key = ('r1', m, q)
                first.setdefault(key, []).append(key + (len(first.get(key, ())),))
                remote(first[key][-1], cut(part[kind], i, where, c0, n), cut(r1[kind], i, where, c0, n), a)

    def service(m, step):
        s, l, kind = m
        i = 2 * s + l
        rows, wide = ROWS[kind], WIDE[kind]
        pa, a1, a2, a3, a4 = part[kind], r1[kind], r2o[kind], r2f[kind], r3[kind]
        key = lambda name, q: (name, m, q)
        if step == 1:
            for q, (c0, n), (a, b, c) in streams(kind):
                for k in first[key('r1', q)]:
                    recv(k)
                fix = {a: pos[a], b: flip[b]}
                remote(key('r2f', q), cut(a1, i, fix, c0, n), cut(a3, i, fix, c0, n), b)
        if step == 2:
            items = []
            for q, (c0, n), (a, b, c) in streams(kind):
                recv(key('r2o', q))
                recv(key('r2f', q))
                fix = {a: pos[a], b: pos[b], c: flip[c]}
                for e, src in enumerate((pa, a1, a2, a3)):
                    items.append((cut(src, i, fix, c0, n), sb[kind].at[e, :, pl.ds(c0, n)]))
            if last_so[kind] is not None:
                for q in range(3):
                    wait_send(('r3', last_so[kind], q))
            last_so[kind] = m
            fetch(kind, items)

            def body(n, carry):
                r = slab(n, SUB)
                v = sb[kind]
                so[kind][r, :] = (v[0, r, :].astype(F32) + v[1, r, :].astype(F32)) + (v[2, r, :].astype(F32) + v[3, r, :].astype(F32))
                return carry
            lax.fori_loop(0, rows // SUB, body, 0)
            for q, (c0, n), (a, b, c) in streams(kind):
                remote(key('r3', q), so[kind].at[:, pl.ds(c0, n)], a4.at[i, :, pl.ds(c0, n)], c)
        if step == 3:
            for q in range(3):
                recv(key('r3', q))
            if kind == 'u' and last_gx[0] is not None:
                wait_send(last_gx[0])
            items = [(src.at[(i,) + spot], sb[kind].at[e]) for e, src in enumerate((pa, a1, a2, a3))]
            fetch(kind, items + [(a4.at[i], r3v[kind])])

            def body(n, carry):
                r = slab(n, SUB)
                v = sb[kind]
                r3v[kind][r, :] = (v[0, r, :].astype(F32) + v[1, r, :].astype(F32)) + (v[2, r, :].astype(F32) + v[3, r, :].astype(F32)) + r3v[kind][r, :]
                return carry
            lax.fori_loop(0, rows // SUB, body, 0)
            if kind == 'd':
                local(r3v[kind], gd.at[i], msem.at[1]).wait()
                spec = pl.BlockSpec((64, D), lambda j: (j, 0))

                def body_d(g, ac, ma, m1, m2, oma, om1, om2, ow):
                    oma[...], om1[...], om2[...] = adam_update(ac[...], g[...], ma[...], m1[...], m2[...])
                    ow[...] = oma[...].astype(BF16)
                pltpu.emit_pipeline(body_d, grid=(4,), in_specs=[spec] * 5, out_specs=[spec] * 4)(
                    gd.at[i], acc['d'].at[s, l], mast['d'].at[s, l], mom1['d'].at[s, l], mom2['d'].at[s, l],
                    nmast['d'].at[s, l], nmom1['d'].at[s, l], nmom2['d'].at[s, l], aw['d'].at[(i,) + spot])
            else:
                last_gx[0] = ('gx', m)
                remote(('gx', m), r3v[kind].at[pl.ds(pl.multiple_of(64 * (1 - core), 64), 64)], gx.at[i], 'core')
                local(r3v[kind].at[pl.ds(pl.multiple_of(64 * core, 64), 64)], go.at[i], msem.at[1]).wait()
        if step == 4:
            recv(('gx', m))
            spec = pl.BlockSpec((64, 512), lambda j: (0, j))
            part_spec = pl.BlockSpec((64, 256), lambda j: (0, j))
            own_spec = pl.BlockSpec((64, 256), lambda j: (core, j))

            def body_u(g0, g1, ac, ma, m1, m2, oma, om1, om2, ow0, ow1):
                low = jnp.where(core == 0, g0[...], g1[...])
                high = jnp.where(core == 0, g1[...], g0[...])
                for h, g in ((0, low), (1, high)):
                    c = slice(256 * h, 256 * h + 256)
                    oma[:, c], om1[:, c], om2[:, c] = adam_update(ac[:, c], g, ma[:, c], m1[:, c], m2[:, c])
                wl, wh = oma[:, :256], oma[:, 256:]
                ow0[...] = jnp.where(core == 0, wl, wh).astype(BF16)
                ow1[...] = jnp.where(core == 0, wh, wl).astype(BF16)
            pltpu.emit_pipeline(body_u, grid=(8,), in_specs=[part_spec] * 2 + [spec] * 4, out_specs=[spec] * 3 + [own_spec, part_spec])(
                go.at[i], gx.at[i], acc['u'].at[s, l], mast['u'].at[s, l], mom1['u'].at[s, l], mom2['u'].at[s, l],
                nmast['u'].at[s, l], nmom1['u'].at[s, l], nmom2['u'].at[s, l], aw['u'].at[(i,) + spot], ws.at[i])
            remote(('ws', m), ws.at[i], aw['u'].at[(i,) + spot + (pl.ds(pl.multiple_of(64 * core, 64), 64),)], 'core')
        if step == 5:
            recv(('ws', m))
        w = aw[kind]
        if (kind == 'd' and step == 3) or step == 5:
            for q, (c0, n), (a, b, c) in streams(kind):
                v = cut(w, i, pos, c0, n)
                remote(key('a1', q), v, v, c)
        if step == 6:
            for q, (c0, n), (a, b, c) in streams(kind):
                recv(key('a1', q))
                v = cut(w, i, {a: pos[a], b: pos[b]}, c0, n)
                remote(key('a2', q), v, v, b)
        if step == 7:
            for q, (c0, n), (a, b, c) in streams(kind):
                recv(key('a2', q))
                v = cut(w, i, {a: pos[a]}, c0, n)
                remote(key('a3', q), v, v, a)

    load_x(0, x_saved.at[0, 1, 0])
    load_w1(0, 1)
    load_y(0, grad_out.at[0, 0])
    load_w2(0, 1)
    barrier = pltpu.get_barrier_semaphore()
    for axis in ('x', 'y', 'z', 'core'):
        pl.semaphore_signal(barrier, inc=1, device_id=(peer[axis],), device_id_type=MESH)
    pl.semaphore_wait(barrier, 4)
    toks = [x_saved.at[0, 1, 0], grad_out.at[0, 0], x_saved.at[0, 0, 0], x_saved.at[1, 1, 0], grad_out.at[1, 0], x_saved.at[1, 0, 0], x_next.at[0, 0], x_next.at[1, 0]]
    xid = {(0, 1): 0, (0, 0): 2, (1, 1): 3, (1, 0): 5}
    for n, src in enumerate(toks):
        remote(('tok', n), src, xr.at[n], 'core')

    following = {(0, 1): (0, 0), (0, 0): (1, 1), (1, 1): (1, 0), (1, 0): None}
    jobs = jobs_of()
    steps = {m: iter(STEPS[m[2]]) for m in MATS.values()}
    for token in ''.join(ORDER):
        if token in MATS:
            service(MATS[token], next(steps[MATS[token]]))
            continue
        name, s, l, half = next(jobs)
        i = 2 * s + l
        nxt = following[s, l]
        own = pl.ds(0, T)
        if name == 'k':
            def arrive():
                recv(('tok', 0))
                load_x(1, xr.at[0])
                recv(('tok', 1))
                load_y(1, xr.at[1])
                ready('xb', 'yb')
            m = (s, l, 'd')
            start = (s, l) == (0, 1)
            if half == 0:
                ready('xa', 'ya', 'w1', 'w2')
                if l == 0:
                    recv(('tk', s))
                    load_y(1, tokr.at[s])
                if not start:
                    ready('xb', 'yb')
            g = half if start else 2 * half
            backward(i, g, 1 if start else 2, arrive if start and half == 0 else None)
            zz, yy = quad(jnp.int32(g))
            g += 0 if start else 1
            send_half('d', m, {'z': zz, 'y': yy} if start else {'z': zz}, 'x')
            if g == 1:
                send_half('d', m, {}, 'z')
            if g == (2 if start else QUADS - 1):
                send_half('d', m, {}, 'y')
            if g == QUADS - 1:
                send_own('d', m)
                if nxt:
                    load_w2(*nxt)
                if l == 0 and nxt:
                    load_w1(*nxt)
                    wait_send(('tk', s))
                    load_y(0, grad_out.at[nxt[0], 0])
                    recv(('tok', 4))
                    load_y(1, xr.at[4])
        elif name == 'bk':
            proj(half, hv, 1 - half, w1v, 1, s if half else None)
            if half == 0:
                load_w1(*nxt)
        elif name == 'j3':
            j3(i, half)
            if half:
                send_half('u', (s, l, 'u'), {})
                send_own('u', (s, l, 'u'))
                n = xid[nxt] if nxt else 6
                load_x(0, x_saved.at[nxt[0], nxt[1], 0] if nxt else x_next.at[0, 0])
                recv(('tok', n))
                load_x(1, xr.at[n])
        elif name == 'cb':
            combine(s, yv)
            remote(('tk', s), yv.at[own], tokr.at[s], 'core')
        elif name == 'f1':
            if half == 1 - l:
                for q in range(3):
                    recv(('a3', (s, l, 'u'), q))
                load_new('u', i)
                if l == 0:
                    ready('xa', 'xb')
                ready('w1')
            elif l:
                recv(('tk', 2 + s))
                load_x(1, tokr.at[2 + s])
                ready('xb')
            f1(half)
        elif name == 'f2':
            if half:
                for q in range(3):
                    recv(('a3', (s, l, 'd'), q))
                load_new('d', i)
                ready('w2')
            proj(half, av, 1 - half, w2v, 0, 2 + i if half else None)
        elif name == 'cf':
            if l:
                wait_send(('tk', 2 + s))
            combine(2 + i, xv)
            if l == 0:
                remote(('tk', 2 + s), xv.at[own], tokr.at[2 + s], 'core')
            else:
                local(xv.at[own], y_out.at[s, 0], msem.at[2]).wait()
                if s == 0:
                    load_x(0, x_next.at[1, 0])
                    recv(('tok', 7))
                    load_x(1, xr.at[7])
    for key in sends:
        wait_send(key)


def solution(mesh):
    tok_spec = P(None, 'fsdp')
    layer_spec = P(None, None, 'fsdp')
    rep_spec = P()

    def device_step(x_saved, grad_out, x_next, w_up, w_down, *state):
        def sds(shape, dtype=F32):
            return jax.ShapeDtypeStruct(shape, dtype)
        up, down = (2, 2, 64, 4096), (2, 2, 256, 1024)
        cube = (4, 2, 2, 2)
        pd, pu = cube + (256, D), cube + (128, H)
        outs = [sds(up), sds(down)] * 3 + [sds((2, 1, T, D), BF16)]
        n_out = len(outs)
        outs += [sds((8, T, D), BF16), sds((4, T, D), BF16), sds((6, T, D))]
        for i in range(4):
            outs += [sds(pd, BF16), sds(pu, BF16)]
        outs += [sds((4, 256, D)), sds((4, 128, H)), sds(pd, BF16), sds(pu, BF16)]
        outs += [sds((4, 256, D)), sds((4, 64, H)), sds((4, 64, H)), sds((4, 64, H), BF16)]
        any_spec = pl.BlockSpec(memory_space=pl.ANY)
        dma = pltpu.SemaphoreType.DMA
        tok_v, hid_v = pltpu.VMEM((2 * T, D), BF16), pltpu.VMEM((2 * T, H), BF16)
        sum_d, sum_u = pltpu.VMEM((256, D), F32), pltpu.VMEM((128, H), F32)
        pair_sem = dma((2,))
        scratch = [
            tok_v, tok_v, pltpu.VMEM((D, H), BF16), pltpu.VMEM((H, D), BF16),
            hid_v, hid_v, pltpu.VMEM((2, T, D), F32),
            pltpu.VMEM((2, 256, D), BF16), pltpu.VMEM((2, 2, 128, H), BF16),
            pltpu.VMEM((4, 256, D), BF16), pltpu.VMEM((4, 128, H), BF16),
            sum_d, sum_u, sum_d, sum_u,
            dma((SEMS,)), dma((SEMS,)), dma((CHIPS,)), dma((CHIPS,)), pair_sem, pair_sem, pair_sem, dma((12,)), dma((3,)),
        ]
        res = pl.pallas_call(
            step_kernel,
            out_shape=outs,
            in_specs=[any_spec] * (5 + len(state)),
            out_specs=[any_spec] * len(outs),
            scratch_shapes=scratch,
            compiler_params=pltpu.CompilerParams(collective_id=0, has_side_effects=True, vmem_limit_bytes=66_900_000),
        )(x_saved, grad_out, x_next, w_up, w_down.reshape(2, 2, 8, 2, 256, D), *state)
        return tuple(res[:n_out])

    return jax.shard_map(device_step, mesh=mesh, in_specs=(layer_spec, tok_spec, tok_spec, rep_spec, rep_spec) + (layer_spec,) * 8, out_specs=(layer_spec,) * 6 + (tok_spec,), check_vma=False)
```

```python
import jax
import jax.numpy as jnp
from jax import lax
from jax.experimental import pallas as pl
from jax.experimental.pallas import tpu as pltpu
from jax.sharding import PartitionSpec as P

LEARN_RATE = 0.005
BETA_ONE = 0.9
BETA_TWO = 0.95
ADAM_EPS = 1e-8
WEIGHT_DECAY = 0.1
MICROBATCHES = 2
ADAM_STEP = 2
F32 = jnp.float32
BF16 = jnp.bfloat16
MESH = pl.DeviceIdType.MESH
GELU_C = 0.7978845608028654
GELU_K = 0.044715
AXES = 'zyx'
ORDERS = ('xyz', 'yzx', 'zxy')
COLS = {'d': ((0, 384), (384, 384), (768, 256)), 'u': ((0, 640), (640, 640), (1280, 768))}
ROWS = {'d': 256, 'u': 128}
WIDE = {'d': 1024, 'u': 2048}
T = 1024
D = 1024
H = 2048
TM = 256
TF = 512
PAIR = (0, 1)
STREAMS = (0, 1, 2)
QUADS = 4
START = (0, 1)
SEMS = 230
TASKS = {'p': ('bk', 1), 'q': ('bk', 0), 'c': ('cb', 0), 'm': ('j3', 0), 'n': ('j3', 1)}
TAIL = ('pqmcn', 'mpqnc')
CHIPS = 8
SUB = 16
LAYERS = 4
VMEM_CAP = 66_900_000
STEPS = {'d': (1, 2, 3, 6, 7), 'u': (1, 2, 3, 4, 5, 6, 7)}
MATS = {}
for s in PAIR:
    for l in reversed(PAIR):
        for kind in 'du':
            MATS['ABCDEFGH'[len(MATS)]] = (s, l, kind)
ORDER = ('jjjjjjAjjAjBjjBjCjjjDjjCjEjDjFjjjBGDEFBCDHAGBDEHDB', 'HCHDGACHBjFjHAjFGjHjFjjjGjFEjjFEjjjjj',)

def adam_update(acc_part, grad_new, master, moment_one, moment_two):
    grad_mean = (acc_part + grad_new) / MICROBATCHES
    moment_one = BETA_ONE * moment_one + (1.0 - BETA_ONE) * grad_mean
    moment_two = BETA_TWO * moment_two + (1.0 - BETA_TWO) * grad_mean * grad_mean
    corr_one = 1.0 - BETA_ONE ** ADAM_STEP
    corr_two = 1.0 - BETA_TWO ** ADAM_STEP
    step_dir = (moment_one / corr_one) / (jnp.sqrt(moment_two / corr_two) + ADAM_EPS)
    master = master - LEARN_RATE * (step_dir + WEIGHT_DECAY * master)
    return master, moment_one, moment_two


def mat(s, l):
    return 2 * s + l


def bit(n):
    return lax.rem(n, 2)


def jobs_of():
    for s in PAIR:
        for l in reversed(PAIR):
            for g in range(3 if (s, l) == START else 2):
                yield 'k', s, l, g
            for token in TAIL[(s, l) == START]:
                name, half = TASKS[token]
                if l or name == 'j3':
                    yield name, s, l, half
    for s in PAIR:
        for l in PAIR:
            for name, half in (('f1', 0), ('f1', 1), ('f2', 1), ('f2', 0), ('cf', 0)):
                if name == 'f1' and half and not l:
                    continue
                if (s, l) != (1, 1) or name == 'f1' or half:
                    yield name, s, l, half


def gelu_parts(h):
    sq = h * h
    th = jnp.tanh(GELU_C * (h + GELU_K * (h * sq)))
    return sq, th


def dot(a, b, ca, cb):
    return lax.dot_general(a, b, (((ca,), (cb,)), ((), ())), preferred_element_type=F32)


def step_kernel(*refs):
    it = iter(refs)
    take = lambda n: [next(it) for i in range(n)]
    x_saved, grad_out, x_next, w_up, w_down = take(5)
    acc, mast, mom1, mom2 = [dict(zip('ud', take(2))) for i in range(4)]
    nmast, nmom1, nmom2 = [dict(zip('ud', take(2))) for i in STREAMS]
    y_out, x_out, a_out = take(3)
    xr, tokr, pr = take(3)
    part, r1, r2o, r2f, r3, aw = [dict(zip('du', take(2))) for i in range(6)]
    gd, go, gx, ws = take(4)
    xv, yv, w1v, w2v, av, hv, fst, dwd, dwu = take(9)
    sb, so, r3v = [dict(zip('du', take(2))) for i in STREAMS]
    ssem, rsem, w1sem, w2sem, xsem, ysem, dwsem, sbsem, msem = take(9)

    me = lax.axis_index('fsdp')
    pos = {'z': lax.div(me, 8), 'y': bit(lax.div(me, 4)), 'x': bit(lax.div(me, 2))}
    core = bit(me)
    flip = {a: 1 - pos[a] for a in AXES}
    peer = {a: me + step * (1 - 2 * pos[a]) for a, step in (('z', 8), ('y', 4), ('x', 2))}
    peer['core'] = me + 1 - 2 * core
    spot = tuple(pos[a] for a in AXES)

    sem_ids = {}
    sends = {}

    def remote(key, src, dst, axis):
        n = sem_ids.setdefault(key, len(sem_ids))
        cp = pltpu.make_async_remote_copy(src_ref=src, dst_ref=dst, send_sem=ssem.at[n], recv_sem=rsem.at[n], device_id=(peer[axis],), device_id_type=MESH)
        cp.start()
        sends[key] = cp

    recv = lambda key: sends[key].wait_recv()
    unsent = set()

    def wait_send(key):
        if key in sends and key not in unsent:
            unsent.add(key)
            sends[key].wait_send()

    def cut(ref, i, fix, c0, n):
        return ref.at[(i,) + tuple(fix.get(a, slice(None)) for a in AXES) + (slice(None), pl.ds(c0, n))]

    def local(src, dst, sem):
        cp = pltpu.make_async_copy(src, dst, sem)
        cp.start()
        return cp

    loads = {'w1': [], 'w2': [], 'xa': [], 'xb': [], 'ya': [], 'yb': []}

    def ready(*names):
        for name in names:
            for cp in loads[name]:
                cp.wait()
            loads[name] = []

    def load_w1(s, l):
        loads['w1'] = [local(w_up.at[s, l, :, pl.ds(512 * c + 256 * core, 256)], w1v.at[:, pl.ds(256 * c, 256)], w1sem.at[c]) for c in range(8)]

    def load_w2(s, l):
        loads['w2'] = [local(w_down.at[s, l, c, core], w2v.at[pl.ds(256 * c, 256)], w2sem.at[c]) for c in range(8)]

    def load_new(kind, i):
        dst, sem, name, rows = (w1v, w1sem, 'w1', 128) if kind == 'u' else (w2v, w2sem, 'w2', 256)
        loads[name] = [local(aw[kind].at[i, c // 4, (c // 2) % 2, c % 2], dst.at[pl.ds(rows * c, rows)], sem.at[c]) for c in range(8)]

    def load_x(half, src):
        loads[('xa', 'xb')[half]] = [local(src, xv.at[pl.ds(T * half, T)], xsem.at[half])]

    def load_y(half, src):
        loads[('ya', 'yb')[half]] = [local(src, yv.at[pl.ds(T * half, T)], ysem.at[half])]

    def slab(n, size):
        return pl.ds(pl.multiple_of(n * size, size), size)

    def quad(g):
        return bit(flip['z'] + lax.div(g, 2)), bit(flip['y'] + g)

    def backward(i, g0, count, hook=None):
        def block(g, hook=None):
            zz, yy = quad(g)
            fs = slab(2 * zz + yy, TF)

            def body(n, carry):
                ts = slab(n, TM)
                h = dot(xv[ts, :], w1v[:, fs], 1, 0)
                da = dot(yv[ts, :], w2v[fs, :], 1, 1)
                sq, th = gelu_parts(h)
                cdf = 0.5 * (1.0 + th)
                av[ts, fs] = (h * cdf).astype(BF16)
                slope = cdf + 0.5 * h * (1.0 - th * th) * (GELU_C * (1.0 + 3.0 * GELU_K * sq))
                hv[ts, fs] = (da * slope).astype(BF16)
                return carry
            tiles = T // TM
            if hook is not None:
                lax.fori_loop(0, tiles, body, 0)
                hook()
                lax.fori_loop(tiles, 2 * tiles, body, 0)
            else:
                lax.fori_loop(0, 2 * tiles, body, 0)

            def out(n):
                return pltpu.make_async_copy(dwd.at[n], part['d'].at[i, zz, yy, n], dwsem.at[n])

            def body2(n, carry):
                f0 = slab(2 * (2 * zz + yy) + n, TM)

                def inner(c, carry):
                    cs = slab(c, TF)
                    dwd[n, :, cs] = dot(av[:, f0], yv[:, cs], 0, 0).astype(BF16)
                    return carry
                lax.fori_loop(0, D // TF, inner, 0)
                out(n).start()
                return carry
            lax.fori_loop(0, 2, body2, 0)
            for n in PAIR:
                out(n).wait()
        if count == 1:
            block(jnp.int32(g0), hook)
        else:
            def each(g, carry):
                block(g)
                return carry
            lax.fori_loop(g0, g0 + count, each, 0)

    def j3(i, half):
        def out(n):
            return pltpu.make_async_copy(dwu.at[n], part['u'].at[i, half, n], dwsem.at[n])

        def body(n, carry):
            def inner(c, carry):
                fs = slab(c, TF)
                res = dot(xv[:, slab(2 * half + n, TM)], hv[:, fs], 0, 0).astype(BF16)
                for e in PAIR:
                    dwu[n, e, :, fs] = res[128 * e:128 * e + 128]
                return carry
            lax.fori_loop(0, H // TF, inner, 0)
            out(n).start()
            return carry
        lax.fori_loop(0, 2, body, 0)
        for n in PAIR:
            out(n).wait()

    def proj(half, src, dst, w, cb, send=None):
        def body(n, carry):
            def inner(c, carry):
                cs = slab(c, TF)
                wt = w[cs, :] if cb else w[:, cs]
                fst[dst, slab(n, TM), cs] = dot(src[slab(T // TM * half + n, TM), :], wt, 1, cb)
                return carry
            return lax.fori_loop(0, D // TF, inner, carry)
        if send is None:
            lax.fori_loop(0, T // TM, body, 0)
            return
        for e in PAIR:
            lax.fori_loop(2 * e, 2 * e + 2, body, 0)
            rows = pl.ds(TF * e, TF)
            remote(('pr', send, e), fst.at[0, rows], pr.at[send, rows], 'core')

    def f1(half, many):
        def body(n, carry):
            ts = slab(T // TM * half + lax.div(n, H // TF), TM)
            fs = slab(lax.rem(n, H // TF), TF)
            h = dot(xv[ts, :], w1v[:, fs], 1, 0)
            sq, th = gelu_parts(h)
            av[ts, fs] = (h * (0.5 * (1.0 + th))).astype(BF16)
            return carry
        lax.fori_loop(0, many * (T // TM) * (H // TF), body, 0)

    def combine(n_pr, base):
        cps = []
        for e in PAIR:
            recv(('pr', n_pr, e))
            wait_send(('pr', n_pr, e))
            rows = pl.ds(TF * e, TF)
            cps.append(local(pr.at[n_pr, rows], fst.at[0, rows], msem.at[2 * e]))
        for e in PAIR:
            cps[e].wait()

            def body(n, carry):
                rows = slab(n, SUB)
                base[rows, :] = (base[rows, :].astype(F32) + (fst[1, rows, :] + fst[0, rows, :])).astype(BF16)
                return carry
            lax.fori_loop(TF * e // SUB, TF * (e + 1) // SUB, body, 0)

    def streams(kind, s):
        return zip(STREAMS, COLS[kind], ORDERS[s:] + ORDERS[:s])

    last_so = {'d': None, 'u': None}
    last_gx = [None]
    first = {}

    def fetch(kind, items):
        cps = [local(src, dst, sbsem.at[n]) for n, (src, dst) in enumerate(items)]
        for cp in cps:
            cp.wait()

    def send_own(kind, m):
        i = mat(*m[:2])
        for q, (c0, n), (a, b, c) in streams(kind, m[0]):
            fix = {a: pos[a], b: flip[b]}
            remote(('r2o', m, q), cut(part[kind], i, fix, c0, n), cut(r2o[kind], i, fix, c0, n), b)

    def send_half(kind, m, fix, which=AXES):
        i = mat(*m[:2])
        for q, (c0, n), (a, b, c) in streams(kind, m[0]):
            if a in which:
                where = {**fix, a: flip[a]}
                key = ('r1', m, q)
                first.setdefault(key, []).append(key + (len(first.get(key, ())),))
                remote(first[key][-1], cut(part[kind], i, where, c0, n), cut(r1[kind], i, where, c0, n), a)

    def service(m, step):
        s, l, kind = m
        i = mat(s, l)
        rows, wide = ROWS[kind], WIDE[kind]
        pa, a1, a2, a3, a4 = part[kind], r1[kind], r2o[kind], r2f[kind], r3[kind]
        key = lambda name, q: (name, m, q)
        if step == 1:
            for q, (c0, n), (a, b, c) in streams(kind, m[0]):
                for k in first[key('r1', q)]:
                    recv(k)
                fix = {a: pos[a], b: flip[b]}
                remote(key('r2f', q), cut(a1, i, fix, c0, n), cut(a3, i, fix, c0, n), b)
        if step == 2:
            items = []
            for q, (c0, n), (a, b, c) in streams(kind, m[0]):
                recv(key('r2o', q))
                recv(key('r2f', q))
                fix = {a: pos[a], b: pos[b], c: flip[c]}
                for e, src in enumerate((pa, a1, a2, a3)):
                    items.append((cut(src, i, fix, c0, n), sb[kind].at[e, :, pl.ds(c0, n)]))
            if last_so[kind] is not None:
                for q in STREAMS:
                    wait_send(('r3', last_so[kind], q))
            last_so[kind] = m
            fetch(kind, items)

            def body(n, carry):
                r = slab(n, SUB)
                v = sb[kind]
                so[kind][r, :] = (v[0, r, :].astype(F32) + v[1, r, :].astype(F32)) + (v[2, r, :].astype(F32) + v[3, r, :].astype(F32))
                return carry
            lax.fori_loop(0, rows // SUB, body, 0)
            for q, (c0, n), (a, b, c) in streams(kind, m[0]):
                remote(key('r3', q), so[kind].at[:, pl.ds(c0, n)], a4.at[i, :, pl.ds(c0, n)], c)
        if step == 3:
            for q in STREAMS:
                recv(key('r3', q))
            if kind == 'u' and last_gx[0] is not None:
                wait_send(last_gx[0])
            items = [(src.at[(i,) + spot], sb[kind].at[e]) for e, src in enumerate((pa, a1, a2, a3))]
            fetch(kind, items + [(a4.at[i], r3v[kind])])

            def body(n, carry):
                r = slab(n, SUB)
                v = sb[kind]
                r3v[kind][r, :] = (v[0, r, :].astype(F32) + v[1, r, :].astype(F32)) + (v[2, r, :].astype(F32) + v[3, r, :].astype(F32)) + r3v[kind][r, :]
                return carry
            lax.fori_loop(0, rows // SUB, body, 0)
            if kind == 'd':
                local(r3v[kind], gd.at[i], msem.at[1]).wait()
                spec = pl.BlockSpec((64, D), lambda j: (j, 0))

                def body_d(g, ac, ma, m1, m2, oma, om1, om2, ow):
                    oma[...], om1[...], om2[...] = adam_update(ac[...], g[...], ma[...], m1[...], m2[...])
                    ow[...] = oma[...].astype(BF16)
                pltpu.emit_pipeline(body_d, grid=(4,), in_specs=[spec] * 5, out_specs=[spec] * 4)(
                    gd.at[i], acc['d'].at[s, l], mast['d'].at[s, l], mom1['d'].at[s, l], mom2['d'].at[s, l],
                    nmast['d'].at[s, l], nmom1['d'].at[s, l], nmom2['d'].at[s, l], aw['d'].at[(i,) + spot])
            else:
                last_gx[0] = ('gx', m)
                remote(('gx', m), r3v[kind].at[pl.ds(pl.multiple_of(64 * (1 - core), 64), 64)], gx.at[i], 'core')
                local(r3v[kind].at[pl.ds(pl.multiple_of(64 * core, 64), 64)], go.at[i], msem.at[1]).wait()
        if step == 4:
            recv(('gx', m))
            spec = pl.BlockSpec((64, 512), lambda j: (0, j))
            part_spec = pl.BlockSpec((64, 256), lambda j: (0, j))
            own_spec = pl.BlockSpec((64, 256), lambda j: (core, j))

            def body_u(g0, g1, ac, ma, m1, m2, oma, om1, om2, ow0, ow1):
                low = jnp.where(core == 0, g0[...], g1[...])
                high = jnp.where(core == 0, g1[...], g0[...])
                for h, g in ((0, low), (1, high)):
                    c = slice(256 * h, 256 * h + 256)
                    oma[:, c], om1[:, c], om2[:, c] = adam_update(ac[:, c], g, ma[:, c], m1[:, c], m2[:, c])
                wl, wh = oma[:, :256], oma[:, 256:]
                ow0[...] = jnp.where(core == 0, wl, wh).astype(BF16)
                ow1[...] = jnp.where(core == 0, wh, wl).astype(BF16)
            pltpu.emit_pipeline(body_u, grid=(8,), in_specs=[part_spec] * 2 + [spec] * 4, out_specs=[spec] * 3 + [own_spec, part_spec])(
                go.at[i], gx.at[i], acc['u'].at[s, l], mast['u'].at[s, l], mom1['u'].at[s, l], mom2['u'].at[s, l],
                nmast['u'].at[s, l], nmom1['u'].at[s, l], nmom2['u'].at[s, l], aw['u'].at[(i,) + spot], ws.at[i])
            remote(('ws', m), ws.at[i], aw['u'].at[(i,) + spot + (pl.ds(pl.multiple_of(64 * core, 64), 64),)], 'core')
        if step == 5:
            recv(('ws', m))
        w = aw[kind]
        if (kind == 'd' and step == 3) or step == 5:
            for q, (c0, n), (a, b, c) in streams(kind, m[0]):
                v = cut(w, i, pos, c0, n)
                remote(key('a1', q), v, v, c)
        if step == 6:
            for q, (c0, n), (a, b, c) in streams(kind, m[0]):
                recv(key('a1', q))
                v = cut(w, i, {a: pos[a], b: pos[b]}, c0, n)
                remote(key('a2', q), v, v, b)
        if step == 7:
            for q, (c0, n), (a, b, c) in streams(kind, m[0]):
                recv(key('a2', q))
                v = cut(w, i, {a: pos[a]}, c0, n)
                remote(key('a3', q), v, v, a)

    load_x(0, x_saved.at[START + (0,)])
    load_w1(*START)
    load_y(0, grad_out.at[0, 0])
    load_w2(*START)
    barrier = pltpu.get_barrier_semaphore()
    for axis in ('x', 'y', 'z', 'core'):
        pl.semaphore_signal(barrier, inc=1, device_id=(peer[axis],), device_id_type=MESH)
    pl.semaphore_wait(barrier, 4)
    toks = [x_saved.at[0, 1, 0], grad_out.at[0, 0], x_saved.at[0, 0, 0], x_saved.at[1, 1, 0], grad_out.at[1, 0], x_saved.at[1, 0, 0], x_next.at[0, 0], x_next.at[1, 0]]
    xid = {(0, 1): 0, (0, 0): 2, (1, 1): 3, (1, 0): 5}
    for n, src in enumerate(toks):
        remote(('tok', n), src, xr.at[n], 'core')

    following = {(0, 1): (0, 0), (0, 0): (1, 1), (1, 1): (1, 0), (1, 0): None}
    jobs = jobs_of()
    steps = {m: iter(STEPS[m[2]]) for m in MATS.values()}
    for token in ''.join(ORDER):
        if token in MATS:
            service(MATS[token], next(steps[MATS[token]]))
            continue
        name, s, l, half = next(jobs)
        i = mat(s, l)
        nxt = following[s, l]
        own = pl.ds(0, T)
        if name == 'k':
            def arrive():
                recv(('tok', 0))
                load_x(1, xr.at[0])
                recv(('tok', 1))
                load_y(1, xr.at[1])
                ready('xb', 'yb')
            m = (s, l, 'd')
            start = (s, l) == START
            if half == 0:
                ready('xa', 'ya', 'w1', 'w2')
                if l == 0:
                    recv(('tk', s))
                    load_y(1, tokr.at[s])
                if not start:
                    ready('xb', 'yb')
            g = half if start else 2 * half
            many = 2 if g == 2 or not start else 1
            backward(i, g, many, arrive if start and half == 0 else None)
            zz, yy = quad(jnp.int32(g))
            last = g + many == QUADS
            which = 'xy' if last else 'xyz' if half == 0 else 'xz'
            send_half('d', m, {'z': zz} if many == 2 else {'z': zz, 'y': yy}, which)
            if last:
                send_own('d', m)
                if nxt:
                    load_w2(*nxt)
                if l == 0 and nxt:
                    load_w1(*nxt)
                    wait_send(('tk', s))
                    load_y(0, grad_out.at[nxt[0], 0])
                    recv(('tok', 4))
                    load_y(1, xr.at[4])
        elif name == 'bk':
            proj(half, hv, 1 - half, w1v, 1, s if half else None)
            if half == 0:
                load_w1(*nxt)
        elif name == 'j3':
            j3(i, half)
            if half:
                send_half('u', (s, l, 'u'), {})
                send_own('u', (s, l, 'u'))
                n = xid[nxt] if nxt else 6
                load_x(0, x_saved.at[nxt[0], nxt[1], 0] if nxt else x_next.at[0, 0])
                recv(('tok', n))
                load_x(1, xr.at[n])
        elif name == 'cb':
            combine(s, yv)
            remote(('tk', s), yv.at[own], tokr.at[s], 'core')
        elif name == 'f1':
            if half == 0:
                for q in STREAMS:
                    recv(('a3', (s, l, 'u'), q))
                load_new('u', i)
                if l == 0:
                    ready('xa', 'xb')
                ready('w1')
            else:
                recv(('tk', 2 + s))
                load_x(1, tokr.at[2 + s])
                ready('xb')
            f1(half, 1 if l else 2)
        elif name == 'f2':
            if half:
                for q in STREAMS:
                    recv(('a3', (s, l, 'd'), q))
                load_new('d', i)
                ready('w2')
            last = (s, l) == (1, 1)
            if last:
                keep = [local(xv.at[own], x_out, msem.at[0]), local(av.at[own], a_out, msem.at[1])]
            proj(half, av, 1 - half, w2v, 0, 2 + i if half else None)
            if last:
                for cp in keep:
                    cp.wait()
                for e in PAIR:
                    recv(('pr', 2 + i, e))
        elif name == 'cf':
            if l:
                wait_send(('tk', 2 + s))
            combine(2 + i, xv)
            if l == 0:
                remote(('tk', 2 + s), xv.at[own], tokr.at[2 + s], 'core')
            else:
                local(xv.at[own], y_out, msem.at[2]).wait()
                load_x(0, x_next.at[1, 0])
                recv(('tok', 7))
                load_x(1, xr.at[7])
    for key in sends:
        wait_send(key)


def finish(*refs):
    states, (y0, x_in, a_in, aw, pr), outs = refs[:6], refs[6:11], refs[11:18]
    stage_u, stage_d, yv, xv, av, wv, pv, isem, osem, lsem = refs[18:]
    last = (LAYERS - 1,)
    loads = [(a_in, av), (x_in, xv), (pr.at[last[0] + 2], pv)]
    for c in range(CHIPS):
        loads.append((aw.at[last + (c // 4, c // 2 % 2, c % 2)], wv.at[pl.ds(256 * c, 256)]))
    loads = [pltpu.make_async_copy(src, dst, lsem.at[n]) for n, (src, dst) in enumerate(loads)]
    moves = [(y0, yv, outs[6].at[0, 0])]
    for n in range(6):
        buf = (stage_u, stage_d)[n % 2]
        for s in PAIR:
            for l in PAIR:
                slot = buf.at[n // 2, s, l]
                moves.append((states[n].at[s, l], slot, outs[n].at[s, l]))
    ins = [pltpu.make_async_copy(a, b, isem.at[n]) for n, (a, b, c) in enumerate(moves)]
    ends = [pltpu.make_async_copy(b, c, osem.at[n]) for n, (a, b, c) in enumerate(moves)]
    for cp in loads + ins:
        cp.start()
    for cp in loads:
        cp.wait()
    tiles = T // TM
    for n in range(tiles):
        rows = pl.ds(n * TM, TM)

        def inner(c, carry):
            cs = pl.ds(pl.multiple_of(c * TF, TF), TF)
            own = dot(av[rows, :], wv[:, cs], 1, 0)
            xv[rows, cs] = (xv[rows, cs].astype(F32) + (own + pv[rows, cs])).astype(BF16)
            return carry
        lax.fori_loop(0, D // TF, inner, 0)
        for k in range(n, len(moves), tiles):
            ins[k].wait()
            ends[k].start()
    out = pltpu.make_async_copy(xv, outs[6].at[1, 0], lsem.at[0])
    out.start()
    for cp in ends + [out]:
        cp.wait()


def solution(mesh):
    tok_spec = P(None, 'fsdp')
    layer_spec = P(None, None, 'fsdp')
    rep_spec = P()

    def device_step(x_saved, grad_out, x_next, w_up, w_down, *state):
        def sds(shape, dtype=F32):
            return jax.ShapeDtypeStruct(shape, dtype)
        up, down = (2, 2, 64, 4096), (2, 2, 256, 1024)
        cube = (4, 2, 2, 2)
        pd, pu = cube + (256, D), cube + (128, H)
        states = [sds(up), sds(down)] * 3
        tok = sds((T, D), BF16)
        outs = states + [tok, tok, sds((T, H), BF16)]
        n_pr = len(outs) + 2
        outs += [sds((CHIPS, T, D), BF16), sds((LAYERS, T, D), BF16), sds((6, T, D))]
        for i in range(4):
            outs += [sds(pd, BF16), sds(pu, BF16)]
        outs += [sds((4, 256, D)), sds((4, 128, H))]
        n_aw = len(outs)
        outs += [sds(pd, BF16), sds(pu, BF16)]
        outs += [sds((4, 256, D)), sds((4, 64, H)), sds((4, 64, H)), sds((4, 64, H), BF16)]
        any_spec = pl.BlockSpec(memory_space=pl.ANY)
        dma = pltpu.SemaphoreType.DMA
        tok_v, hid_v = pltpu.VMEM((2 * T, D), BF16), pltpu.VMEM((2 * T, H), BF16)
        sum_d, sum_u = pltpu.VMEM((256, D), F32), pltpu.VMEM((128, H), F32)
        pair_sem = dma((2,))
        scratch = [
            tok_v, tok_v, pltpu.VMEM((D, H), BF16), pltpu.VMEM((H, D), BF16),
            hid_v, hid_v, pltpu.VMEM((2, T, D), F32),
            pltpu.VMEM((2, 256, D), BF16), pltpu.VMEM((2, 2, 128, H), BF16),
            pltpu.VMEM((4, 256, D), BF16), pltpu.VMEM((4, 128, H), BF16),
            sum_d, sum_u, sum_d, sum_u,
            dma((SEMS,)), dma((SEMS,)), dma((CHIPS,)), dma((CHIPS,)), pair_sem, pair_sem, pair_sem, dma((12,)), dma((3,)),
        ]
        res = pl.pallas_call(
            step_kernel,
            out_shape=outs,
            in_specs=[any_spec] * (5 + len(state)),
            out_specs=[any_spec] * len(outs),
            scratch_shapes=scratch,
            compiler_params=pltpu.CompilerParams(collective_id=0, has_side_effects=True, vmem_limit_bytes=VMEM_CAP),
        )(x_saved, grad_out, x_next, w_up, w_down.reshape(2, 2, 8, 2, 256, D), *state)
        vm = pltpu.VMEM
        final = pl.pallas_call(
            finish,
            out_shape=states + [sds((2, 1, T, D), BF16)],
            in_specs=[any_spec] * 11,
            out_specs=[any_spec] * 7,
            scratch_shapes=[vm((3,) + up, F32), vm((3,) + down, F32), vm((T, D), BF16), vm((T, D), BF16), vm((T, H), BF16), vm((H, D), BF16), vm((T, D), F32), dma((32,)), dma((32,)), dma((12,))],
            compiler_params=pltpu.CompilerParams(vmem_limit_bytes=VMEM_CAP),
        )(*res[:9], res[n_aw], res[n_pr])
        return tuple(final)

    return jax.shard_map(device_step, mesh=mesh, in_specs=(layer_spec, tok_spec, tok_spec, rep_spec, rep_spec) + (layer_spec,) * 8, out_specs=(layer_spec,) * 6 + (tok_spec,), check_vma=False)
```

```python
import jax
import jax.numpy as jnp
from jax import lax
from jax.experimental import pallas as pl
from jax.experimental.pallas import tpu as pltpu
from jax.sharding import PartitionSpec as P

LEARN_RATE = 0.005
BETA_ONE = 0.9
BETA_TWO = 0.95
ADAM_EPS = 1e-8
WEIGHT_DECAY = 0.1
MICROBATCHES = 2
ADAM_STEP = 2
F32 = jnp.float32
BF16 = jnp.bfloat16
MESH = pl.DeviceIdType.MESH
GELU_C = 0.7978845608028654
GELU_K = 0.044715
AXES = 'zyx'
ORDERS = ('xyz', 'yzx', 'zxy')
COLS = {'d': ((0, 384), (384, 384), (768, 256)), 'u': ((0, 640), (640, 640), (1280, 768))}
ROWS = {'d': 256, 'u': 128}
WIDE = {'d': 1024, 'u': 2048}
T = 1024
D = 1024
H = 2048
TM = 256
TF = 512
PAIR = (0, 1)
STREAMS = (0, 1, 2)
QUADS = 4
START = (0, 1)
LAST = (1, 1, 'd')
SEMS = 240
TASKS = {'p': ('bk', 1), 'q': ('bk', 0), 'c': ('cb', 0), 'm': ('j3', 0), 'n': ('j3', 1)}
TAIL = ('pqmcn', 'mpqnc')
CHIPS = 8
SUB = 16
LAYERS = 4
VMEM_CAP = 66_900_000
STEPS = {'d': (1, 2, 3, 6, 7), 'u': (1, 2, 3, 4, 5, 6, 7)}
MATS = {}
for s in PAIR:
    for l in reversed(PAIR):
        for kind in 'du':
            MATS['ABCDEFGH'[len(MATS)]] = (s, l, kind)
ORDER = ('jjjjjjAjjAjBjBjCjjCjjjDjEjjjDFjjEjDBDCGFBDHAGDBECH', 'FBAFDHHCGHBjHjGAjjjFHjjGFEjjjFjEjjjjj',)

def adam_update(acc_part, grad_new, master, moment_one, moment_two):
    grad_mean = (acc_part + grad_new) / MICROBATCHES
    moment_one = BETA_ONE * moment_one + (1.0 - BETA_ONE) * grad_mean
    moment_two = BETA_TWO * moment_two + (1.0 - BETA_TWO) * grad_mean * grad_mean
    corr_one = 1.0 - BETA_ONE ** ADAM_STEP
    corr_two = 1.0 - BETA_TWO ** ADAM_STEP
    step_dir = (moment_one / corr_one) / (jnp.sqrt(moment_two / corr_two) + ADAM_EPS)
    master = master - LEARN_RATE * (step_dir + WEIGHT_DECAY * master)
    return master, moment_one, moment_two


def mat(s, l):
    return 2 * s + l


def bit(n):
    return lax.rem(n, 2)


def jobs_of():
    for s in PAIR:
        for l in reversed(PAIR):
            for g in range(3 if (s, l) == START else 2):
                yield 'k', s, l, g
            for token in TAIL[(s, l) == START]:
                name, half = TASKS[token]
                if l or name == 'j3':
                    yield name, s, l, half
    for s in PAIR:
        for l in PAIR:
            for name, half in (('f1', 0), ('f1', 1), ('f2', 1), ('f2', 0), ('cf', 0)):
                if name == 'f1' and half and not l:
                    continue
                if (s, l) != LAST[:2] or name == 'f1' or (name, half) == ('f2', 1):
                    yield name, s, l, half


def gelu_parts(h):
    sq = h * h
    th = jnp.tanh(GELU_C * (h + GELU_K * (h * sq)))
    return sq, th


def dot(a, b, ca, cb):
    return lax.dot_general(a, b, (((ca,), (cb,)), ((), ())), preferred_element_type=F32)


def step_kernel(*refs):
    it = iter(refs)
    take = lambda n: [next(it) for i in range(n)]
    x_saved, grad_out, x_next, w_up, w_down = take(5)
    acc, mast, mom1, mom2 = [dict(zip('ud', take(2))) for i in range(4)]
    nmast, nmom1, nmom2 = [dict(zip('ud', take(2))) for i in STREAMS]
    y_out, x_out, a_out, a_far, w_far = take(5)
    xr, tokr, pr = take(3)
    part, r1, r2o, r2f, r3, aw = [dict(zip('du', take(2))) for i in range(6)]
    gd, go, gx, ws = take(4)
    xv, yv, w1v, w2v, av, hv, fst, dwd, dwu = take(9)
    sb, so, r3v = [dict(zip('du', take(2))) for i in STREAMS]
    ssem, rsem, w1sem, w2sem, xsem, ysem, dwsem, sbsem, msem = take(9)

    me = lax.axis_index('fsdp')
    pos = {'z': lax.div(me, 8), 'y': bit(lax.div(me, 4)), 'x': bit(lax.div(me, 2))}
    core = bit(me)
    flip = {a: 1 - pos[a] for a in AXES}
    peer = {a: me + step * (1 - 2 * pos[a]) for a, step in (('z', 8), ('y', 4), ('x', 2))}
    peer['core'] = me + 1 - 2 * core
    spot = tuple(pos[a] for a in AXES)

    sem_ids = {}
    sends = {}

    def remote(key, src, dst, axis):
        n = sem_ids.setdefault(key, len(sem_ids))
        cp = pltpu.make_async_remote_copy(src_ref=src, dst_ref=dst, send_sem=ssem.at[n], recv_sem=rsem.at[n], device_id=(peer[axis],), device_id_type=MESH)
        cp.start()
        sends[key] = cp

    recv = lambda key: sends[key].wait_recv()
    unsent = set()

    def wait_send(key):
        if key in sends and key not in unsent:
            unsent.add(key)
            sends[key].wait_send()

    def cut(ref, i, fix, c0, n):
        return ref.at[(i,) + tuple(fix.get(a, slice(None)) for a in AXES) + (slice(None), pl.ds(c0, n))]

    def local(src, dst, sem):
        cp = pltpu.make_async_copy(src, dst, sem)
        cp.start()
        return cp

    loads = {'w1': [], 'w2': [], 'xa': [], 'xb': [], 'ya': [], 'yb': []}

    def ready(*names):
        for name in names:
            for cp in loads[name]:
                cp.wait()
            loads[name] = []

    def load_w1(s, l):
        loads['w1'] = [local(w_up.at[s, l, :, pl.ds(512 * c + 256 * core, 256)], w1v.at[:, pl.ds(256 * c, 256)], w1sem.at[c]) for c in range(8)]

    def load_w2(s, l):
        loads['w2'] = [local(w_down.at[s, l, c, core], w2v.at[pl.ds(256 * c, 256)], w2sem.at[c]) for c in range(8)]

    def load_new(kind, i):
        dst, sem, name, rows = (w1v, w1sem, 'w1', 128) if kind == 'u' else (w2v, w2sem, 'w2', 256)
        loads[name] = [local(aw[kind].at[i, c // 4, (c // 2) % 2, c % 2], dst.at[pl.ds(rows * c, rows)], sem.at[c]) for c in range(8)]

    def load_x(half, src):
        loads[('xa', 'xb')[half]] = [local(src, xv.at[pl.ds(T * half, T)], xsem.at[half])]

    def load_y(half, src):
        loads[('ya', 'yb')[half]] = [local(src, yv.at[pl.ds(T * half, T)], ysem.at[half])]

    def slab(n, size):
        return pl.ds(pl.multiple_of(n * size, size), size)

    def quad(g):
        return bit(flip['z'] + lax.div(g, 2)), bit(flip['y'] + g)

    def backward(i, g0, count, hook=None):
        def block(g, hook=None):
            zz, yy = quad(g)
            fs = slab(2 * zz + yy, TF)

            def body(n, carry):
                ts = slab(n, TM)
                h = dot(xv[ts, :], w1v[:, fs], 1, 0)
                da = dot(yv[ts, :], w2v[fs, :], 1, 1)
                sq, th = gelu_parts(h)
                cdf = 0.5 * (1.0 + th)
                av[ts, fs] = (h * cdf).astype(BF16)
                slope = cdf + 0.5 * h * (1.0 - th * th) * (GELU_C * (1.0 + 3.0 * GELU_K * sq))
                hv[ts, fs] = (da * slope).astype(BF16)
                return carry
            tiles = T // TM
            if hook is not None:
                lax.fori_loop(0, tiles, body, 0)
                hook()
                lax.fori_loop(tiles, 2 * tiles, body, 0)
            else:
                lax.fori_loop(0, 2 * tiles, body, 0)

            def out(n):
                return pltpu.make_async_copy(dwd.at[n], part['d'].at[i, zz, yy, n], dwsem.at[n])

            def body2(n, carry):
                f0 = slab(2 * (2 * zz + yy) + n, TM)

                def inner(c, carry):
                    cs = slab(c, TF)
                    dwd[n, :, cs] = dot(av[:, f0], yv[:, cs], 0, 0).astype(BF16)
                    return carry
                lax.fori_loop(0, D // TF, inner, 0)
                out(n).start()
                return carry
            lax.fori_loop(0, 2, body2, 0)
            for n in PAIR:
                out(n).wait()
        if count == 1:
            block(jnp.int32(g0), hook)
        else:
            def each(g, carry):
                block(g)
                return carry
            lax.fori_loop(g0, g0 + count, each, 0)

    def j3(i, half):
        def out(n):
            return pltpu.make_async_copy(dwu.at[n], part['u'].at[i, half, n], dwsem.at[n])

        def body(n, carry):
            def inner(c, carry):
                fs = slab(c, TF)
                res = dot(xv[:, slab(2 * half + n, TM)], hv[:, fs], 0, 0).astype(BF16)
                for e in PAIR:
                    dwu[n, e, :, fs] = res[128 * e:128 * e + 128]
                return carry
            lax.fori_loop(0, H // TF, inner, 0)
            out(n).start()
            return carry
        lax.fori_loop(0, 2, body, 0)
        for n in PAIR:
            out(n).wait()

    def proj(half, src, dst, w, cb, send=None):
        def body(n, carry):
            def inner(c, carry):
                cs = slab(c, TF)
                wt = w[cs, :] if cb else w[:, cs]
                fst[dst, slab(n, TM), cs] = dot(src[slab(T // TM * half + n, TM), :], wt, 1, cb)
                return carry
            return lax.fori_loop(0, D // TF, inner, carry)
        if send is None:
            lax.fori_loop(0, T // TM, body, 0)
            return
        for e in PAIR:
            lax.fori_loop(2 * e, 2 * e + 2, body, 0)
            rows = pl.ds(TF * e, TF)
            remote(('pr', send, e), fst.at[0, rows], pr.at[send, rows], 'core')

    def f1(half, many):
        def body(n, carry):
            ts = slab(T // TM * half + lax.div(n, H // TF), TM)
            fs = slab(lax.rem(n, H // TF), TF)
            h = dot(xv[ts, :], w1v[:, fs], 1, 0)
            sq, th = gelu_parts(h)
            av[ts, fs] = (h * (0.5 * (1.0 + th))).astype(BF16)
            return carry
        lax.fori_loop(0, many * (T // TM) * (H // TF), body, 0)

    def combine(n_pr, base):
        cps = []
        for e in PAIR:
            recv(('pr', n_pr, e))
            wait_send(('pr', n_pr, e))
            rows = pl.ds(TF * e, TF)
            cps.append(local(pr.at[n_pr, rows], fst.at[0, rows], msem.at[2 * e]))
        for e in PAIR:
            cps[e].wait()

            def body(n, carry):
                rows = slab(n, SUB)
                base[rows, :] = (base[rows, :].astype(F32) + (fst[1, rows, :] + fst[0, rows, :])).astype(BF16)
                return carry
            lax.fori_loop(TF * e // SUB, TF * (e + 1) // SUB, body, 0)

    def streams(kind, m):
        r = mat(*m[:2]) % len(ORDERS)
        return zip(STREAMS, COLS[kind], ORDERS[r:] + ORDERS[:r])

    last_so = {'d': None, 'u': None}
    last_gx = [None]
    first = {}

    def fetch(kind, items):
        cps = [local(src, dst, sbsem.at[n]) for n, (src, dst) in enumerate(items)]
        for cp in cps:
            cp.wait()

    def send_own(kind, m):
        i = mat(*m[:2])
        for q, (c0, n), (a, b, c) in streams(kind, m):
            fix = {a: pos[a], b: flip[b]}
            remote(('r2o', m, q), cut(part[kind], i, fix, c0, n), cut(r2o[kind], i, fix, c0, n), b)

    def send_half(kind, m, fix, which=AXES):
        i = mat(*m[:2])
        for q, (c0, n), (a, b, c) in streams(kind, m):
            if a in which:
                where = {**fix, a: flip[a]}
                key = ('r1', m, q)
                first.setdefault(key, []).append(key + (len(first.get(key, ())),))
                remote(first[key][-1], cut(part[kind], i, where, c0, n), cut(r1[kind], i, where, c0, n), a)

    def far_half(fix, q, c0, n):
        i = mat(*LAST[:2])
        part_of = lambda ref: ref.at[tuple(fix.get(a, slice(None)) for a in AXES) + (slice(None), pl.ds(c0, n))]
        key = ('far', q)
        first.setdefault(key, []).append(key + (len(first.get(key, ())),))
        remote(first[key][-1], cut(aw['d'], i, fix, c0, n), part_of(w_far), 'core')

    def service(m, step):
        s, l, kind = m
        i = mat(s, l)
        rows, wide = ROWS[kind], WIDE[kind]
        pa, a1, a2, a3, a4 = part[kind], r1[kind], r2o[kind], r2f[kind], r3[kind]
        key = lambda name, q: (name, m, q)
        if step == 1:
            for q, (c0, n), (a, b, c) in streams(kind, m):
                for k in first[key('r1', q)]:
                    recv(k)
                fix = {a: pos[a], b: flip[b]}
                remote(key('r2f', q), cut(a1, i, fix, c0, n), cut(a3, i, fix, c0, n), b)
        if step == 2:
            items = []
            for q, (c0, n), (a, b, c) in streams(kind, m):
                recv(key('r2o', q))
                recv(key('r2f', q))
                fix = {a: pos[a], b: pos[b], c: flip[c]}
                for e, src in enumerate((pa, a1, a2, a3)):
                    items.append((cut(src, i, fix, c0, n), sb[kind].at[e, :, pl.ds(c0, n)]))
            if last_so[kind] is not None:
                for q in STREAMS:
                    wait_send(('r3', last_so[kind], q))
            last_so[kind] = m
            fetch(kind, items)

            def body(n, carry):
                r = slab(n, SUB)
                v = sb[kind]
                so[kind][r, :] = (v[0, r, :].astype(F32) + v[1, r, :].astype(F32)) + (v[2, r, :].astype(F32) + v[3, r, :].astype(F32))
                return carry
            lax.fori_loop(0, rows // SUB, body, 0)
            for q, (c0, n), (a, b, c) in streams(kind, m):
                remote(key('r3', q), so[kind].at[:, pl.ds(c0, n)], a4.at[i, :, pl.ds(c0, n)], c)
        if step == 3:
            for q in STREAMS:
                recv(key('r3', q))
            if kind == 'u' and last_gx[0] is not None:
                wait_send(last_gx[0])
            items = [(src.at[(i,) + spot], sb[kind].at[e]) for e, src in enumerate((pa, a1, a2, a3))]
            fetch(kind, items + [(a4.at[i], r3v[kind])])

            def body(n, carry):
                r = slab(n, SUB)
                v = sb[kind]
                r3v[kind][r, :] = (v[0, r, :].astype(F32) + v[1, r, :].astype(F32)) + (v[2, r, :].astype(F32) + v[3, r, :].astype(F32)) + r3v[kind][r, :]
                return carry
            lax.fori_loop(0, rows // SUB, body, 0)
            if kind == 'd':
                local(r3v[kind], gd.at[i], msem.at[1]).wait()
                spec = pl.BlockSpec((64, D), lambda j: (j, 0))

                def body_d(g, ac, ma, m1, m2, oma, om1, om2, ow):
                    oma[...], om1[...], om2[...] = adam_update(ac[...], g[...], ma[...], m1[...], m2[...])
                    ow[...] = oma[...].astype(BF16)
                pltpu.emit_pipeline(body_d, grid=(4,), in_specs=[spec] * 5, out_specs=[spec] * 4)(
                    gd.at[i], acc['d'].at[s, l], mast['d'].at[s, l], mom1['d'].at[s, l], mom2['d'].at[s, l],
                    nmast['d'].at[s, l], nmom1['d'].at[s, l], nmom2['d'].at[s, l], aw['d'].at[(i,) + spot])
            else:
                last_gx[0] = ('gx', m)
                remote(('gx', m), r3v[kind].at[pl.ds(pl.multiple_of(64 * (1 - core), 64), 64)], gx.at[i], 'core')
                local(r3v[kind].at[pl.ds(pl.multiple_of(64 * core, 64), 64)], go.at[i], msem.at[1]).wait()
        if step == 4:
            recv(('gx', m))
            spec = pl.BlockSpec((64, 512), lambda j: (0, j))
            part_spec = pl.BlockSpec((64, 256), lambda j: (0, j))
            own_spec = pl.BlockSpec((64, 256), lambda j: (core, j))

            def body_u(g0, g1, ac, ma, m1, m2, oma, om1, om2, ow0, ow1):
                low = jnp.where(core == 0, g0[...], g1[...])
                high = jnp.where(core == 0, g1[...], g0[...])
                for h, g in ((0, low), (1, high)):
                    c = slice(256 * h, 256 * h + 256)
                    oma[:, c], om1[:, c], om2[:, c] = adam_update(ac[:, c], g, ma[:, c], m1[:, c], m2[:, c])
                wl, wh = oma[:, :256], oma[:, 256:]
                ow0[...] = jnp.where(core == 0, wl, wh).astype(BF16)
                ow1[...] = jnp.where(core == 0, wh, wl).astype(BF16)
            pltpu.emit_pipeline(body_u, grid=(8,), in_specs=[part_spec] * 2 + [spec] * 4, out_specs=[spec] * 3 + [own_spec, part_spec])(
                go.at[i], gx.at[i], acc['u'].at[s, l], mast['u'].at[s, l], mom1['u'].at[s, l], mom2['u'].at[s, l],
                nmast['u'].at[s, l], nmom1['u'].at[s, l], nmom2['u'].at[s, l], aw['u'].at[(i,) + spot], ws.at[i])
            remote(('ws', m), ws.at[i], aw['u'].at[(i,) + spot + (pl.ds(pl.multiple_of(64 * core, 64), 64),)], 'core')
        if step == 5:
            recv(('ws', m))
        w = aw[kind]
        if (kind == 'd' and step == 3) or step == 5:
            for q, (c0, n), (a, b, c) in streams(kind, m):
                v = cut(w, i, pos, c0, n)
                remote(key('a1', q), v, v, c)
        if step == 6:
            for q, (c0, n), (a, b, c) in streams(kind, m):
                recv(key('a1', q))
                v = cut(w, i, {a: pos[a], b: pos[b]}, c0, n)
                remote(key('a2', q), v, v, b)
        if step == 7:
            for q, (c0, n), (a, b, c) in streams(kind, m):
                recv(key('a2', q))
                v = cut(w, i, {a: pos[a]}, c0, n)
                remote(key('a3', q), v, v, a)
                if m == LAST:
                    far_half({a: pos[a]}, q, c0, n)

    load_x(0, x_saved.at[START + (0,)])
    load_w1(*START)
    load_y(0, grad_out.at[0, 0])
    load_w2(*START)
    barrier = pltpu.get_barrier_semaphore()
    for axis in ('x', 'y', 'z', 'core'):
        pl.semaphore_signal(barrier, inc=1, device_id=(peer[axis],), device_id_type=MESH)
    pl.semaphore_wait(barrier, 4)
    toks = [x_saved.at[0, 1, 0], grad_out.at[0, 0], x_saved.at[0, 0, 0], x_saved.at[1, 1, 0], grad_out.at[1, 0], x_saved.at[1, 0, 0], x_next.at[0, 0], x_next.at[1, 0]]
    xid = {(0, 1): 0, (0, 0): 2, (1, 1): 3, (1, 0): 5}
    for n, src in enumerate(toks):
        remote(('tok', n), src, (xv, yv)[n].at[pl.ds(T, T)] if n < 2 else xr.at[n], 'core')

    following = {(0, 1): (0, 0), (0, 0): (1, 1), (1, 1): (1, 0), (1, 0): None}
    jobs = jobs_of()
    steps = {m: iter(STEPS[m[2]]) for m in MATS.values()}
    for token in ''.join(ORDER):
        if token in MATS:
            service(MATS[token], next(steps[MATS[token]]))
            continue
        name, s, l, half = next(jobs)
        i = mat(s, l)
        nxt = following[s, l]
        own = pl.ds(0, T)
        if name == 'k':
            def arrive():
                for n in PAIR:
                    recv(('tok', n))
            m = (s, l, 'd')
            start = (s, l) == START
            if half == 0:
                ready('xa', 'ya', 'w1', 'w2')
                if l == 0:
                    recv(('tk', s))
                    load_y(1, tokr.at[s])
                if not start:
                    ready('xb', 'yb')
            g = half if start else 2 * half
            many = 2 if g == 2 or not start else 1
            backward(i, g, many, arrive if start and half == 0 else None)
            zz, yy = quad(jnp.int32(g))
            last = g + many == QUADS
            which = 'xy' if last else 'xyz' if half == 0 else 'xz'
            send_half('d', m, {'z': zz} if many == 2 else {'z': zz, 'y': yy}, which)
            if last:
                send_own('d', m)
                if nxt:
                    load_w2(*nxt)
                if l == 0 and nxt:
                    load_w1(*nxt)
                    wait_send(('tk', s))
                    load_y(0, grad_out.at[nxt[0], 0])
                    recv(('tok', 4))
                    load_y(1, xr.at[4])
        elif name == 'bk':
            proj(half, hv, 1 - half, w1v, 1, s if half else None)
            if half == 0:
                load_w1(*nxt)
        elif name == 'j3':
            j3(i, half)
            if half:
                send_half('u', (s, l, 'u'), {})
                send_own('u', (s, l, 'u'))
                n = xid[nxt] if nxt else 6
                load_x(0, x_saved.at[nxt[0], nxt[1], 0] if nxt else x_next.at[0, 0])
                recv(('tok', n))
                load_x(1, xr.at[n])
        elif name == 'cb':
            combine(s, yv)
            remote(('tk', s), yv.at[own], tokr.at[s], 'core')
        elif name == 'f1':
            if half == 0:
                for q in STREAMS:
                    recv(('a3', (s, l, 'u'), q))
                load_new('u', i)
                if l == 0:
                    ready('xa', 'xb')
                ready('w1')
            else:
                recv(('tk', 2 + s))
                load_x(1, tokr.at[2 + s])
                ready('xb')
            f1(half, 1 if l else 2)
            if (s, l) == LAST[:2]:
                if half:
                    remote('a_far', av.at[pl.ds(T, T)], a_far, 'core')
                else:
                    keep = [local(xv.at[own], x_out, msem.at[0]), local(av.at[own], a_out, msem.at[1])]
        elif name == 'f2' and (s, l) == LAST[:2]:
            for q, (c0, n), (a, b, c) in streams('d', LAST):
                recv(('a3', LAST, q))
                far_half({a: flip[a]}, q, c0, n)
            for cp in keep:
                cp.wait()
            for q in STREAMS:
                for k in first['far', q]:
                    recv(k)
            recv('a_far')
        elif name == 'f2':
            if half:
                for q in STREAMS:
                    recv(('a3', (s, l, 'd'), q))
                load_new('d', i)
                ready('w2')
            proj(half, av, 1 - half, w2v, 0, 2 + i if half else None)
        elif name == 'cf':
            if l:
                wait_send(('tk', 2 + s))
            combine(2 + i, xv)
            if l == 0:
                remote(('tk', 2 + s), xv.at[own], tokr.at[2 + s], 'core')
            else:
                local(xv.at[own], y_out, msem.at[2]).wait()
                load_x(0, x_next.at[1, 0])
                recv(('tok', 7))
                load_x(1, xr.at[7])
    for key in sends:
        wait_send(key)


def finish(*refs):
    states, (y0, x_in, a_in, a_far, w_far, aw), outs = refs[:6], refs[6:12], refs[12:19]
    stage_u, stage_d, yv, xv, av, wv, isem, osem, lsem = refs[19:]
    last = (LAYERS - 1,)
    loads = [(x_in, xv), (a_in, av.at[0]), (a_far, av.at[1])]
    for c in range(CHIPS):
        spot = (c // 4, c // 2 % 2, c % 2)
        for e, src in enumerate((aw.at[last + spot], w_far.at[spot])):
            loads.append((src, wv.at[e, pl.ds(256 * c, 256)]))
    loads = [pltpu.make_async_copy(src, dst, lsem.at[n]) for n, (src, dst) in enumerate(loads)]
    moves = [(y0, yv, outs[6].at[0, 0])]
    for n in range(6):
        buf = (stage_u, stage_d)[n % 2]
        for s in PAIR:
            for l in PAIR:
                slot = buf.at[n // 2, s, l]
                moves.append((states[n].at[s, l], slot, outs[n].at[s, l]))
    ins = [pltpu.make_async_copy(a, b, isem.at[n]) for n, (a, b, c) in enumerate(moves)]
    ends = [pltpu.make_async_copy(b, c, osem.at[n]) for n, (a, b, c) in enumerate(moves)]
    for cp in loads + ins:
        cp.start()
    for cp in loads:
        cp.wait()
    def tile(n, carry):
        rows = pl.ds(pl.multiple_of(n * TM, TM), TM)

        def inner(c, carry):
            cs = pl.ds(pl.multiple_of(c * TF, TF), TF)
            mlp = dot(av[0, rows, :], wv[0, :, cs], 1, 0) + dot(av[1, rows, :], wv[1, :, cs], 1, 0)
            xv[rows, cs] = (xv[rows, cs].astype(F32) + mlp).astype(BF16)
            return carry
        return lax.fori_loop(0, D // TF, inner, carry)
    group = T // TM // len(PAIR)
    for g in PAIR:
        lax.fori_loop(group * g, group * (g + 1), tile, 0)
        for k in range(g, len(moves), len(PAIR)):
            ins[k].wait()
            ends[k].start()
    out = pltpu.make_async_copy(xv, outs[6].at[1, 0], lsem.at[0])
    out.start()
    for cp in ends + [out]:
        cp.wait()


def solution(mesh):
    tok_spec = P(None, 'fsdp')
    layer_spec = P(None, None, 'fsdp')
    rep_spec = P()

    def device_step(x_saved, grad_out, x_next, w_up, w_down, *state):
        def sds(shape, dtype=F32):
            return jax.ShapeDtypeStruct(shape, dtype)
        up, down = (2, 2, 64, 4096), (2, 2, 256, 1024)
        cube = (4, 2, 2, 2)
        pd, pu = cube + (256, D), cube + (128, H)
        states = [sds(up), sds(down)] * 3
        tok = sds((T, D), BF16)
        hid = sds((T, H), BF16)
        outs = states + [tok, tok, hid, hid, sds((2, 2, 2, 256, D), BF16)]
        n_main = len(outs)
        outs += [sds((CHIPS, T, D), BF16), sds((LAYERS, T, D), BF16), sds((6, T, D))]
        for i in range(4):
            outs += [sds(pd, BF16), sds(pu, BF16)]
        outs += [sds((4, 256, D)), sds((4, 128, H))]
        n_aw = len(outs)
        outs += [sds(pd, BF16), sds(pu, BF16)]
        outs += [sds((4, 256, D)), sds((4, 64, H)), sds((4, 64, H)), sds((4, 64, H), BF16)]
        any_spec = pl.BlockSpec(memory_space=pl.ANY)
        dma = pltpu.SemaphoreType.DMA
        tok_v, hid_v = pltpu.VMEM((2 * T, D), BF16), pltpu.VMEM((2 * T, H), BF16)
        sum_d, sum_u = pltpu.VMEM((256, D), F32), pltpu.VMEM((128, H), F32)
        pair_sem = dma((2,))
        scratch = [
            tok_v, tok_v, pltpu.VMEM((D, H), BF16), pltpu.VMEM((H, D), BF16),
            hid_v, hid_v, pltpu.VMEM((2, T, D), F32),
            pltpu.VMEM((2, 256, D), BF16), pltpu.VMEM((2, 2, 128, H), BF16),
            pltpu.VMEM((4, 256, D), BF16), pltpu.VMEM((4, 128, H), BF16),
            sum_d, sum_u, sum_d, sum_u,
            dma((SEMS,)), dma((SEMS,)), dma((CHIPS,)), dma((CHIPS,)), pair_sem, pair_sem, pair_sem, dma((12,)), dma((3,)),
        ]
        res = pl.pallas_call(
            step_kernel,
            out_shape=outs,
            in_specs=[any_spec] * (5 + len(state)),
            out_specs=[any_spec] * len(outs),
            scratch_shapes=scratch,
            compiler_params=pltpu.CompilerParams(collective_id=0, has_side_effects=True, vmem_limit_bytes=VMEM_CAP),
        )(x_saved, grad_out, x_next, w_up, w_down.reshape(2, 2, 8, 2, 256, D), *state)
        vm = pltpu.VMEM
        final = pl.pallas_call(
            finish,
            out_shape=states + [sds((2, 1, T, D), BF16)],
            in_specs=[any_spec] * 12,
            out_specs=[any_spec] * 7,
            scratch_shapes=[vm((3,) + up, F32), vm((3,) + down, F32), vm((T, D), BF16), vm((T, D), BF16), vm((2, T, H), BF16), vm((2, H, D), BF16), dma((32,)), dma((32,)), dma((32,))],
            compiler_params=pltpu.CompilerParams(vmem_limit_bytes=VMEM_CAP),
        )(*res[:n_main], res[n_aw])
        return tuple(final)

    return jax.shard_map(device_step, mesh=mesh, in_specs=(layer_spec, tok_spec, tok_spec, rep_spec, rep_spec) + (layer_spec,) * 8, out_specs=(layer_spec,) * 6 + (tok_spec,), check_vma=False)
```

```python
import jax
import jax.numpy as jnp
from jax import lax
from jax.experimental import pallas as pl
from jax.experimental.pallas import tpu as pltpu
from jax.sharding import PartitionSpec as P

LEARN_RATE = 0.005
BETA_ONE = 0.9
BETA_TWO = 0.95
ADAM_EPS = 1e-8
WEIGHT_DECAY = 0.1
MICROBATCHES = 2
ADAM_STEP = 2
F32 = jnp.float32
BF16 = jnp.bfloat16
MESH = pl.DeviceIdType.MESH
GELU_C = 0.7978845608028654
GELU_K = 0.044715
AXES = 'zyx'
ORDERS = ('xyz', 'yzx', 'zxy')
COLS = {'d': ((0, 384), (384, 384), (768, 256)), 'u': ((0, 640), (640, 640), (1280, 768))}
ROWS = {'d': 256, 'u': 128}
WIDE = {'d': 1024, 'u': 2048}
T = 1024
D = 1024
H = 2048
TM = 256
TF = 512
PAIR = (0, 1)
STREAMS = (0, 1, 2)
QUADS = 4
START = (0, 1)
LAST = (1, 1, 'd')
SEMS = 240
TASKS = {'p': ('bk', 1), 'q': ('bk', 0), 'c': ('cb', 0), 'm': ('j3', 0), 'n': ('j3', 1)}
TAIL = ('pqmcn', 'mpqnc')
CHIPS = 8
SUB = 16
LAYERS = 4
VMEM_CAP = 66_900_000
STEPS = {'d': (1, 2, 3, 6, 7), 'u': (1, 2, 3, 4, 5, 6, 7)}
MATS = {}
for s in PAIR:
    for l in reversed(PAIR):
        for kind in 'du':
            MATS['ABCDEFGH'[len(MATS)]] = (s, l, kind)
ORDER = ('jjjjjjAjjAjBjBjCjjCjjjDjEjjjDFjjEjDBDCGFBDHAGDBECH', 'FBAFDHHCGHBjHjGAjjjFHjjGFEjjjFjEjjjjj',)

def adam_update(acc_part, grad_new, master, moment_one, moment_two):
    grad_mean = (acc_part + grad_new) / MICROBATCHES
    moment_one = BETA_ONE * moment_one + (1.0 - BETA_ONE) * grad_mean
    moment_two = BETA_TWO * moment_two + (1.0 - BETA_TWO) * grad_mean * grad_mean
    corr_one = 1.0 - BETA_ONE ** ADAM_STEP
    corr_two = 1.0 - BETA_TWO ** ADAM_STEP
    step_dir = (moment_one / corr_one) / (jnp.sqrt(moment_two / corr_two) + ADAM_EPS)
    master = master - LEARN_RATE * (step_dir + WEIGHT_DECAY * master)
    return master, moment_one, moment_two


def mat(s, l):
    return 2 * s + l


def bit(n):
    return lax.rem(n, 2)


def jobs_of():
    for s in PAIR:
        for l in reversed(PAIR):
            for g in range(3 if (s, l) == START else 2):
                yield 'k', s, l, g
            for token in TAIL[(s, l) == START]:
                name, half = TASKS[token]
                if l or name == 'j3':
                    yield name, s, l, half
    for s in PAIR:
        for l in PAIR:
            for name, half in (('f1', 0), ('f1', 1), ('f2', 1), ('f2', 0), ('cf', 0)):
                if name == 'f1' and half and not l:
                    continue
                if (s, l) != LAST[:2] or name == 'f1' or (name, half) == ('f2', 1):
                    yield name, s, l, half


def gelu_parts(h):
    sq = h * h
    th = jnp.tanh(GELU_C * (h + GELU_K * (h * sq)))
    return sq, th


def dot(a, b, ca, cb):
    return lax.dot_general(a, b, (((ca,), (cb,)), ((), ())), preferred_element_type=F32)


def step_kernel(*refs):
    it = iter(refs)
    take = lambda n: [next(it) for i in range(n)]
    x_saved, grad_out, x_next, w_up, w_down = take(5)
    acc, mast, mom1, mom2 = [dict(zip('ud', take(2))) for i in range(4)]
    nmast, nmom1, nmom2 = [dict(zip('ud', take(2))) for i in STREAMS]
    y_out, x_out, a_out, a_far, w_far = take(5)
    xr, tokr, pr = take(3)
    part, r1, r2o, r2f, r3, aw = [dict(zip('du', take(2))) for i in range(6)]
    gd, go, gx, ws = take(4)
    xv, yv, w1v, w2v, av, hv, fst, dwd, dwu = take(9)
    sb, so, r3v = [dict(zip('du', take(2))) for i in STREAMS]
    ssem, rsem, w1sem, w2sem, xsem, ysem, dwsem, sbsem, msem = take(9)

    me = lax.axis_index('fsdp')
    pos = {'z': lax.div(me, 8), 'y': bit(lax.div(me, 4)), 'x': bit(lax.div(me, 2))}
    core = bit(me)
    flip = {a: 1 - pos[a] for a in AXES}
    peer = {a: me + step * (1 - 2 * pos[a]) for a, step in (('z', 8), ('y', 4), ('x', 2))}
    peer['core'] = me + 1 - 2 * core
    spot = tuple(pos[a] for a in AXES)

    sem_ids = {}
    sends = {}

    def remote(key, src, dst, axis):
        n = sem_ids.setdefault(key, len(sem_ids))
        cp = pltpu.make_async_remote_copy(src_ref=src, dst_ref=dst, send_sem=ssem.at[n], recv_sem=rsem.at[n], device_id=(peer[axis],), device_id_type=MESH)
        cp.start()
        sends[key] = cp

    recv = lambda key: sends[key].wait_recv()
    unsent = set()

    def wait_send(key):
        if key in sends and key not in unsent:
            unsent.add(key)
            sends[key].wait_send()

    def cut(ref, i, fix, c0, n):
        return ref.at[(i,) + tuple(fix.get(a, slice(None)) for a in AXES) + (slice(None), pl.ds(c0, n))]

    def local(src, dst, sem):
        cp = pltpu.make_async_copy(src, dst, sem)
        cp.start()
        return cp

    loads = {'w1': [], 'w2': [], 'xa': [], 'xb': [], 'ya': [], 'yb': []}

    def ready(*names):
        for name in names:
            for cp in loads[name]:
                cp.wait()
            loads[name] = []

    def load_w1(s, l):
        loads['w1'] = [local(w_up.at[s, l, :, pl.ds(512 * c + 256 * core, 256)], w1v.at[:, pl.ds(256 * c, 256)], w1sem.at[c]) for c in range(8)]

    def load_w2(s, l):
        loads['w2'] = [local(w_down.at[s, l, c, core], w2v.at[pl.ds(256 * c, 256)], w2sem.at[c]) for c in range(8)]

    def load_new(kind, i):
        dst, sem, name, rows = (w1v, w1sem, 'w1', 128) if kind == 'u' else (w2v, w2sem, 'w2', 256)
        loads[name] = [local(aw[kind].at[i, c // 4, (c // 2) % 2, c % 2], dst.at[pl.ds(rows * c, rows)], sem.at[c]) for c in range(8)]

    def load_x(half, src):
        loads[('xa', 'xb')[half]] = [local(src, xv.at[pl.ds(T * half, T)], xsem.at[half])]

    def load_y(half, src):
        loads[('ya', 'yb')[half]] = [local(src, yv.at[pl.ds(T * half, T)], ysem.at[half])]

    def slab(n, size):
        return pl.ds(pl.multiple_of(n * size, size), size)

    def quad(g):
        return bit(flip['z'] + lax.div(g, 2)), bit(flip['y'] + g)

    def backward(i, g0, count, hook=None):
        def block(g, hook=None):
            zz, yy = quad(g)
            fs = slab(2 * zz + yy, TF)

            def body(n, carry):
                ts = slab(n, TM)
                h = dot(xv[ts, :], w1v[:, fs], 1, 0)
                da = dot(yv[ts, :], w2v[fs, :], 1, 1)
                sq, th = gelu_parts(h)
                cdf = 0.5 * (1.0 + th)
                av[ts, fs] = (h * cdf).astype(BF16)
                slope = cdf + 0.5 * h * (1.0 - th * th) * (GELU_C * (1.0 + 3.0 * GELU_K * sq))
                hv[ts, fs] = (da * slope).astype(BF16)
                return carry
            tiles = T // TM
            if hook is not None:
                lax.fori_loop(0, tiles, body, 0)
                hook()
                lax.fori_loop(tiles, 2 * tiles, body, 0)
            else:
                lax.fori_loop(0, 2 * tiles, body, 0)

            def out(n):
                return pltpu.make_async_copy(dwd.at[n], part['d'].at[i, zz, yy, n], dwsem.at[n])

            def body2(n, carry):
                f0 = slab(2 * (2 * zz + yy) + n, TM)

                def inner(c, carry):
                    cs = slab(c, TF)
                    dwd[n, :, cs] = dot(av[:, f0], yv[:, cs], 0, 0).astype(BF16)
                    return carry
                lax.fori_loop(0, D // TF, inner, 0)
                out(n).start()
                return carry
            lax.fori_loop(0, 2, body2, 0)
            for n in PAIR:
                out(n).wait()
        if count == 1:
            block(jnp.int32(g0), hook)
        else:
            def each(g, carry):
                block(g)
                return carry
            lax.fori_loop(g0, g0 + count, each, 0)

    def j3(i, half):
        def out(n):
            return pltpu.make_async_copy(dwu.at[n], part['u'].at[i, half, n], dwsem.at[n])

        def body(n, carry):
            def inner(c, carry):
                fs = slab(c, TF)
                res = dot(xv[:, slab(2 * half + n, TM)], hv[:, fs], 0, 0).astype(BF16)
                for e in PAIR:
                    dwu[n, e, :, fs] = res[128 * e:128 * e + 128]
                return carry
            lax.fori_loop(0, H // TF, inner, 0)
            out(n).start()
            return carry
        lax.fori_loop(0, 2, body, 0)
        for n in PAIR:
            out(n).wait()

    def proj(half, src, dst, w, cb, send=None):
        def body(n, carry):
            def inner(c, carry):
                cs = slab(c, TF)
                wt = w[cs, :] if cb else w[:, cs]
                fst[dst, slab(n, TM), cs] = dot(src[slab(T // TM * half + n, TM), :], wt, 1, cb)
                return carry
            return lax.fori_loop(0, D // TF, inner, carry)
        if send is None:
            lax.fori_loop(0, T // TM, body, 0)
            return
        for e in PAIR:
            lax.fori_loop(2 * e, 2 * e + 2, body, 0)
            rows = pl.ds(TF * e, TF)
            remote(('pr', send, e), fst.at[0, rows], pr.at[send, rows], 'core')

    def f1(half, many):
        def body(n, carry):
            ts = slab(T // TM * half + lax.div(n, H // TF), TM)
            fs = slab(lax.rem(n, H // TF), TF)
            h = dot(xv[ts, :], w1v[:, fs], 1, 0)
            sq, th = gelu_parts(h)
            av[ts, fs] = (h * (0.5 * (1.0 + th))).astype(BF16)
            return carry
        lax.fori_loop(0, many * (T // TM) * (H // TF), body, 0)

    def combine(n_pr, base):
        cps = []
        for e in PAIR:
            recv(('pr', n_pr, e))
            wait_send(('pr', n_pr, e))
            rows = pl.ds(TF * e, TF)
            cps.append(local(pr.at[n_pr, rows], fst.at[0, rows], msem.at[2 * e]))
        for e in PAIR:
            cps[e].wait()

            def body(n, carry):
                rows = slab(n, SUB)
                base[rows, :] = (base[rows, :].astype(F32) + (fst[1, rows, :] + fst[0, rows, :])).astype(BF16)
                return carry
            lax.fori_loop(TF * e // SUB, TF * (e + 1) // SUB, body, 0)

    def streams(kind, m):
        r = mat(*m[:2]) % len(ORDERS)
        return zip(STREAMS, COLS[kind], ORDERS[r:] + ORDERS[:r])

    last_so = {'d': None, 'u': None}
    last_gx = [None]
    first = {}

    def fetch(kind, items):
        cps = [local(src, dst, sbsem.at[n]) for n, (src, dst) in enumerate(items)]
        for cp in cps:
            cp.wait()

    def send_own(kind, m):
        i = mat(*m[:2])
        for q, (c0, n), (a, b, c) in streams(kind, m):
            fix = {a: pos[a], b: flip[b]}
            remote(('r2o', m, q), cut(part[kind], i, fix, c0, n), cut(r2o[kind], i, fix, c0, n), b)

    def send_half(kind, m, fix, which=AXES):
        i = mat(*m[:2])
        for q, (c0, n), (a, b, c) in streams(kind, m):
            if a in which:
                where = {**fix, a: flip[a]}
                key = ('r1', m, q)
                first.setdefault(key, []).append(key + (len(first.get(key, ())),))
                remote(first[key][-1], cut(part[kind], i, where, c0, n), cut(r1[kind], i, where, c0, n), a)

    def far_half(fix, q, c0, n):
        i = mat(*LAST[:2])
        part_of = lambda ref: ref.at[tuple(fix.get(a, slice(None)) for a in AXES) + (slice(None), pl.ds(c0, n))]
        key = ('far', q)
        first.setdefault(key, []).append(key + (len(first.get(key, ())),))
        remote(first[key][-1], cut(aw['d'], i, fix, c0, n), part_of(w_far), 'core')

    def service(m, step):
        s, l, kind = m
        i = mat(s, l)
        rows, wide = ROWS[kind], WIDE[kind]
        pa, a1, a2, a3, a4 = part[kind], r1[kind], r2o[kind], r2f[kind], r3[kind]
        key = lambda name, q: (name, m, q)
        if step == 1:
            for q, (c0, n), (a, b, c) in streams(kind, m):
                for k in first[key('r1', q)]:
                    recv(k)
                fix = {a: pos[a], b: flip[b]}
                remote(key('r2f', q), cut(a1, i, fix, c0, n), cut(a3, i, fix, c0, n), b)
        if step == 2:
            items = []
            for q, (c0, n), (a, b, c) in streams(kind, m):
                recv(key('r2o', q))
                recv(key('r2f', q))
                fix = {a: pos[a], b: pos[b], c: flip[c]}
                for e, src in enumerate((pa, a1, a2, a3)):
                    items.append((cut(src, i, fix, c0, n), sb[kind].at[e, :, pl.ds(c0, n)]))
            if last_so[kind] is not None:
                for q in STREAMS:
                    wait_send(('r3', last_so[kind], q))
            last_so[kind] = m
            fetch(kind, items)

            def body(n, carry):
                r = slab(n, SUB)
                v = sb[kind]
                so[kind][r, :] = (v[0, r, :].astype(F32) + v[1, r, :].astype(F32)) + (v[2, r, :].astype(F32) + v[3, r, :].astype(F32))
                return carry
            lax.fori_loop(0, rows // SUB, body, 0)
            for q, (c0, n), (a, b, c) in streams(kind, m):
                remote(key('r3', q), so[kind].at[:, pl.ds(c0, n)], a4.at[i, :, pl.ds(c0, n)], c)
        if step == 3:
            for q in STREAMS:
                recv(key('r3', q))
            if kind == 'u' and last_gx[0] is not None:
                wait_send(last_gx[0])
            items = [(src.at[(i,) + spot], sb[kind].at[e]) for e, src in enumerate((pa, a1, a2, a3))]
            fetch(kind, items + [(a4.at[i], r3v[kind])])

            def body(n, carry):
                r = slab(n, SUB)
                v = sb[kind]
                r3v[kind][r, :] = (v[0, r, :].astype(F32) + v[1, r, :].astype(F32)) + (v[2, r, :].astype(F32) + v[3, r, :].astype(F32)) + r3v[kind][r, :]
                return carry
            lax.fori_loop(0, rows // SUB, body, 0)
            if kind == 'd':
                local(r3v[kind], gd.at[i], msem.at[1]).wait()
                spec = pl.BlockSpec((64, D), lambda j: (j, 0))

                def body_d(g, ac, ma, m1, m2, oma, om1, om2, ow):
                    oma[...], om1[...], om2[...] = adam_update(ac[...], g[...], ma[...], m1[...], m2[...])
                    ow[...] = oma[...].astype(BF16)
                pltpu.emit_pipeline(body_d, grid=(4,), in_specs=[spec] * 5, out_specs=[spec] * 4)(
                    gd.at[i], acc['d'].at[s, l], mast['d'].at[s, l], mom1['d'].at[s, l], mom2['d'].at[s, l],
                    nmast['d'].at[s, l], nmom1['d'].at[s, l], nmom2['d'].at[s, l], aw['d'].at[(i,) + spot])
            else:
                last_gx[0] = ('gx', m)
                remote(('gx', m), r3v[kind].at[pl.ds(pl.multiple_of(64 * (1 - core), 64), 64)], gx.at[i], 'core')
                local(r3v[kind].at[pl.ds(pl.multiple_of(64 * core, 64), 64)], go.at[i], msem.at[1]).wait()
        if step == 4:
            recv(('gx', m))
            spec = pl.BlockSpec((64, 512), lambda j: (0, j))
            part_spec = pl.BlockSpec((64, 256), lambda j: (0, j))
            own_spec = pl.BlockSpec((64, 256), lambda j: (core, j))

            def body_u(g0, g1, ac, ma, m1, m2, oma, om1, om2, ow0, ow1):
                low = jnp.where(core == 0, g0[...], g1[...])
                high = jnp.where(core == 0, g1[...], g0[...])
                for h, g in ((0, low), (1, high)):
                    c = slice(256 * h, 256 * h + 256)
                    oma[:, c], om1[:, c], om2[:, c] = adam_update(ac[:, c], g, ma[:, c], m1[:, c], m2[:, c])
                wl, wh = oma[:, :256], oma[:, 256:]
                ow0[...] = jnp.where(core == 0, wl, wh).astype(BF16)
                ow1[...] = jnp.where(core == 0, wh, wl).astype(BF16)
            pltpu.emit_pipeline(body_u, grid=(8,), in_specs=[part_spec] * 2 + [spec] * 4, out_specs=[spec] * 3 + [own_spec, part_spec])(
                go.at[i], gx.at[i], acc['u'].at[s, l], mast['u'].at[s, l], mom1['u'].at[s, l], mom2['u'].at[s, l],
                nmast['u'].at[s, l], nmom1['u'].at[s, l], nmom2['u'].at[s, l], aw['u'].at[(i,) + spot], ws.at[i])
            remote(('ws', m), ws.at[i], aw['u'].at[(i,) + spot + (pl.ds(pl.multiple_of(64 * core, 64), 64),)], 'core')
        if step == 5:
            recv(('ws', m))
        w = aw[kind]
        if (kind == 'd' and step == 3) or step == 5:
            for q, (c0, n), (a, b, c) in streams(kind, m):
                v = cut(w, i, pos, c0, n)
                remote(key('a1', q), v, v, c)
        if step == 6:
            for q, (c0, n), (a, b, c) in streams(kind, m):
                recv(key('a1', q))
                v = cut(w, i, {a: pos[a], b: pos[b]}, c0, n)
                remote(key('a2', q), v, v, b)
        if step == 7:
            for q, (c0, n), (a, b, c) in streams(kind, m):
                recv(key('a2', q))
                v = cut(w, i, {a: pos[a]}, c0, n)
                remote(key('a3', q), v, v, a)
                if m == LAST:
                    far_half({a: pos[a]}, q, c0, n)

    load_x(0, x_saved.at[START + (0,)])
    load_w1(*START)
    load_y(0, grad_out.at[0, 0])
    load_w2(*START)
    barrier = pltpu.get_barrier_semaphore()
    for axis in ('x', 'y', 'z', 'core'):
        pl.semaphore_signal(barrier, inc=1, device_id=(peer[axis],), device_id_type=MESH)
    pl.semaphore_wait(barrier, 4)
    toks = [x_saved.at[0, 1, 0], grad_out.at[0, 0], x_saved.at[0, 0, 0], x_saved.at[1, 1, 0], grad_out.at[1, 0], x_saved.at[1, 0, 0], x_next.at[0, 0], x_next.at[1, 0]]
    xid = {(0, 1): 0, (0, 0): 2, (1, 1): 3, (1, 0): 5}
    for n, src in enumerate(toks):
        remote(('tok', n), src, (xv, yv)[n].at[pl.ds(T, T)] if n < 2 else xr.at[n], 'core')

    following = {(0, 1): (0, 0), (0, 0): (1, 1), (1, 1): (1, 0), (1, 0): None}
    jobs = jobs_of()
    steps = {m: iter(STEPS[m[2]]) for m in MATS.values()}
    for token in ''.join(ORDER):
        if token in MATS:
            service(MATS[token], next(steps[MATS[token]]))
            continue
        name, s, l, half = next(jobs)
        i = mat(s, l)
        nxt = following[s, l]
        own = pl.ds(0, T)
        if name == 'k':
            def arrive():
                for n in PAIR:
                    recv(('tok', n))
            m = (s, l, 'd')
            start = (s, l) == START
            if half == 0:
                ready('xa', 'ya', 'w1', 'w2')
                if l == 0:
                    recv(('tk', s))
                    load_y(1, tokr.at[s])
                if not start:
                    ready('xb', 'yb')
            g = half if start else 2 * half
            many = 2 if g == 2 or not start else 1
            backward(i, g, many, arrive if start and half == 0 else None)
            zz, yy = quad(jnp.int32(g))
            last = g + many == QUADS
            which = 'xy' if last else 'xyz' if half == 0 else 'xz'
            send_half('d', m, {'z': zz} if many == 2 else {'z': zz, 'y': yy}, which)
            if last:
                send_own('d', m)
                if nxt:
                    load_w2(*nxt)
                if l == 0 and nxt:
                    load_w1(*nxt)
                    wait_send(('tk', s))
                    load_y(0, grad_out.at[nxt[0], 0])
                    recv(('tok', 4))
                    load_y(1, xr.at[4])
        elif name == 'bk':
            proj(half, hv, 1 - half, w1v, 1, s if half else None)
            if half == 0:
                load_w1(*nxt)
        elif name == 'j3':
            j3(i, half)
            if half:
                send_half('u', (s, l, 'u'), {})
                send_own('u', (s, l, 'u'))
                n = xid[nxt] if nxt else 6
                load_x(0, x_saved.at[nxt[0], nxt[1], 0] if nxt else x_next.at[0, 0])
                recv(('tok', n))
                load_x(1, xr.at[n])
        elif name == 'cb':
            combine(s, yv)
            remote(('tk', s), yv.at[own], tokr.at[s], 'core')
        elif name == 'f1':
            if half == 0:
                for q in STREAMS:
                    recv(('a3', (s, l, 'u'), q))
                load_new('u', i)
                if l == 0:
                    ready('xa', 'xb')
                ready('w1')
            else:
                recv(('tk', 2 + s))
                load_x(1, tokr.at[2 + s])
                ready('xb')
            f1(half, 1 if l else 2)
            if (s, l) == LAST[:2]:
                if half:
                    remote('a_far', av.at[pl.ds(T, T)], a_far, 'core')
                else:
                    keep = [local(xv.at[own], x_out, msem.at[0]), local(av.at[own], a_out, msem.at[1])]
        elif name == 'f2' and (s, l) == LAST[:2]:
            for q, (c0, n), (a, b, c) in streams('d', LAST):
                recv(('a3', LAST, q))
                far_half({a: flip[a]}, q, c0, n)
            for cp in keep:
                cp.wait()
            for q in STREAMS:
                for k in first['far', q]:
                    recv(k)
            recv('a_far')
        elif name == 'f2':
            if half:
                for q in STREAMS:
                    recv(('a3', (s, l, 'd'), q))
                load_new('d', i)
                ready('w2')
            proj(half, av, 1 - half, w2v, 0, 2 + i if half else None)
        elif name == 'cf':
            if l:
                wait_send(('tk', 2 + s))
            combine(2 + i, xv)
            if l == 0:
                remote(('tk', 2 + s), xv.at[own], tokr.at[2 + s], 'core')
            else:
                local(xv.at[own], y_out, msem.at[2]).wait()
                load_x(0, x_next.at[1, 0])
                recv(('tok', 7))
                load_x(1, xr.at[7])
    for key in sends:
        wait_send(key)


def finish(*refs):
    states, (y0, x_in, a_in, a_far, w_far, aw), outs = refs[:6], refs[6:12], refs[12:19]
    stage_u, stage_d, yv, xv, av, wv, isem, osem, lsem = refs[19:]
    last = (LAYERS - 1,)
    loads = [(x_in, xv), (a_in, av.at[0]), (a_far, av.at[1])]
    for c in range(CHIPS):
        spot = (c // 4, c // 2 % 2, c % 2)
        for e, src in enumerate((aw.at[last + spot], w_far.at[spot])):
            loads.append((src, wv.at[e, pl.ds(256 * c, 256)]))
    loads = [pltpu.make_async_copy(src, dst, lsem.at[n]) for n, (src, dst) in enumerate(loads)]
    moves = [(y0, yv, outs[6].at[0, 0])]
    for n in range(6):
        buf = (stage_u, stage_d)[n % 2]
        for s in PAIR:
            for l in PAIR:
                slot = buf.at[n // 2, s, l]
                moves.append((states[n].at[s, l], slot, outs[n].at[s, l]))
    ins = [pltpu.make_async_copy(a, b, isem.at[n]) for n, (a, b, c) in enumerate(moves)]
    ends = [pltpu.make_async_copy(b, c, osem.at[n]) for n, (a, b, c) in enumerate(moves)]
    for cp in loads + ins:
        cp.start()
    for cp in loads:
        cp.wait()
    def tile(n, carry):
        rows = pl.ds(n * TM, TM)

        def inner(c, carry):
            cs = pl.ds(pl.multiple_of(c * TM, TM), TM)
            mlp = dot(av[0, rows, :], wv[0, :, cs], 1, 0) + dot(av[1, rows, :], wv[1, :, cs], 1, 0)
            xv[rows, cs] = (xv[rows, cs].astype(F32) + mlp).astype(BF16)
            return carry
        return lax.fori_loop(0, D // TM, inner, carry)
    tiles = T // TM
    share = len(moves) // tiles
    for n in range(tiles):
        tile(n, 0)
        for k in range(share * n, len(moves) if n == tiles - 1 else share * n + share):
            ins[k].wait()
            ends[k].start()
    out = pltpu.make_async_copy(xv, outs[6].at[1, 0], lsem.at[0])
    out.start()
    for cp in ends + [out]:
        cp.wait()


def solution(mesh):
    tok_spec = P(None, 'fsdp')
    layer_spec = P(None, None, 'fsdp')
    rep_spec = P()

    def device_step(x_saved, grad_out, x_next, w_up, w_down, *state):
        def sds(shape, dtype=F32):
            return jax.ShapeDtypeStruct(shape, dtype)
        up, down = (2, 2, 64, 4096), (2, 2, 256, 1024)
        cube = (4, 2, 2, 2)
        pd, pu = cube + (256, D), cube + (128, H)
        states = [sds(up), sds(down)] * 3
        tok = sds((T, D), BF16)
        hid = sds((T, H), BF16)
        outs = states + [tok, tok, hid, hid, sds((2, 2, 2, 256, D), BF16)]
        n_main = len(outs)
        outs += [sds((CHIPS, T, D), BF16), sds((LAYERS, T, D), BF16), sds((6, T, D))]
        for i in range(4):
            outs += [sds(pd, BF16), sds(pu, BF16)]
        outs += [sds((4, 256, D)), sds((4, 128, H))]
        n_aw = len(outs)
        outs += [sds(pd, BF16), sds(pu, BF16)]
        outs += [sds((4, 256, D)), sds((4, 64, H)), sds((4, 64, H)), sds((4, 64, H), BF16)]
        any_spec = pl.BlockSpec(memory_space=pl.ANY)
        dma = pltpu.SemaphoreType.DMA
        tok_v, hid_v = pltpu.VMEM((2 * T, D), BF16), pltpu.VMEM((2 * T, H), BF16)
        sum_d, sum_u = pltpu.VMEM((256, D), F32), pltpu.VMEM((128, H), F32)
        pair_sem = dma((2,))
        scratch = [
            tok_v, tok_v, pltpu.VMEM((D, H), BF16), pltpu.VMEM((H, D), BF16),
            hid_v, hid_v, pltpu.VMEM((2, T, D), F32),
            pltpu.VMEM((2, 256, D), BF16), pltpu.VMEM((2, 2, 128, H), BF16),
            pltpu.VMEM((4, 256, D), BF16), pltpu.VMEM((4, 128, H), BF16),
            sum_d, sum_u, sum_d, sum_u,
            dma((SEMS,)), dma((SEMS,)), dma((CHIPS,)), dma((CHIPS,)), pair_sem, pair_sem, pair_sem, dma((12,)), dma((3,)),
        ]
        res = pl.pallas_call(
            step_kernel,
            out_shape=outs,
            in_specs=[any_spec] * (5 + len(state)),
            out_specs=[any_spec] * len(outs),
            scratch_shapes=scratch,
            compiler_params=pltpu.CompilerParams(collective_id=0, has_side_effects=True, vmem_limit_bytes=VMEM_CAP),
        )(x_saved, grad_out, x_next, w_up, w_down.reshape(2, 2, 8, 2, 256, D), *state)
        vm = pltpu.VMEM
        final = pl.pallas_call(
            finish,
            out_shape=states + [sds((2, 1, T, D), BF16)],
            in_specs=[any_spec] * 12,
            out_specs=[any_spec] * 7,
            scratch_shapes=[vm((3,) + up, F32), vm((3,) + down, F32), vm((T, D), BF16), vm((T, D), BF16), vm((2, T, H), BF16), vm((2, H, D), BF16), dma((32,)), dma((32,)), dma((32,))],
            compiler_params=pltpu.CompilerParams(vmem_limit_bytes=VMEM_CAP),
        )(*res[:n_main], res[n_aw])
        return tuple(final)

    return jax.shard_map(device_step, mesh=mesh, in_specs=(layer_spec, tok_spec, tok_spec, rep_spec, rep_spec) + (layer_spec,) * 8, out_specs=(layer_spec,) * 6 + (tok_spec,), check_vma=False)
```

```python
import jax
import jax.numpy as jnp
from jax import lax
from jax.experimental import pallas as pl
from jax.experimental.pallas import tpu as pltpu
from jax.sharding import PartitionSpec as P

LEARN_RATE = 0.005
BETA_ONE = 0.9
BETA_TWO = 0.95
ADAM_EPS = 1e-8
WEIGHT_DECAY = 0.1
MICROBATCHES = 2
ADAM_STEP = 2
F32 = jnp.float32
BF16 = jnp.bfloat16
MESH = pl.DeviceIdType.MESH
GELU_C = 0.7978845608028654
GELU_K = 0.044715
AXES = 'zyx'
ORDERS = ('xyz', 'yzx', 'zxy')
COLS = {'d': ((0, 384), (384, 384), (768, 256)), 'u': ((0, 640), (640, 640), (1280, 768))}
ROWS = {'d': 256, 'u': 128}
WIDE = {'d': 1024, 'u': 2048}
T = 1024
D = 1024
H = 2048
TM = 256
TF = 512
PAIR = (0, 1)
STREAMS = (0, 1, 2)
QUADS = 4
START = (0, 1)
LAST = (1, 1, 'd')
SEMS = 240
TASKS = {'p': ('bk', 1), 'q': ('bk', 0), 'c': ('cb', 0), 'm': ('j3', 0), 'n': ('j3', 1)}
TAIL = ('pqmcn', 'mpqnc')
CHIPS = 8
SUB = 16
LAYERS = 4
VMEM_CAP = 66_900_000
STEPS = {'d': (1, 2, 3, 6, 7), 'u': (1, 2, 3, 4, 5, 6, 7)}
MATS = {}
for s in PAIR:
    for l in reversed(PAIR):
        for kind in 'du':
            MATS['ABCDEFGH'[len(MATS)]] = (s, l, kind)
ORDER = ('jjjjjjAjjAjBjBjCjjCjjjDjEjjjDFjjEjDBDCGFBDHAGDBECH', 'FBAFDHHCGHBjHjGAjjjFHjjGFEjjjFjEjjjjj',)

def adam_update(acc_part, grad_new, master, moment_one, moment_two):
    grad_mean = (acc_part + grad_new) / MICROBATCHES
    moment_one = BETA_ONE * moment_one + (1.0 - BETA_ONE) * grad_mean
    moment_two = BETA_TWO * moment_two + (1.0 - BETA_TWO) * grad_mean * grad_mean
    corr_one = 1.0 - BETA_ONE ** ADAM_STEP
    corr_two = 1.0 - BETA_TWO ** ADAM_STEP
    step_dir = (moment_one / corr_one) / (jnp.sqrt(moment_two / corr_two) + ADAM_EPS)
    master = master - LEARN_RATE * (step_dir + WEIGHT_DECAY * master)
    return master, moment_one, moment_two


def mat(s, l):
    return 2 * s + l


def bit(n):
    return lax.rem(n, 2)


def jobs_of():
    for s in PAIR:
        for l in reversed(PAIR):
            for g in range(3 if (s, l) == START else 2):
                yield 'k', s, l, g
            for token in TAIL[(s, l) == START]:
                name, half = TASKS[token]
                if l or name == 'j3':
                    yield name, s, l, half
    for s in PAIR:
        for l in PAIR:
            for name, half in (('f1', 0), ('f1', 1), ('f2', 1), ('f2', 0), ('cf', 0)):
                if name == 'f1' and half and not l:
                    continue
                if (s, l) != LAST[:2] or name == 'f1' or (name, half) == ('f2', 1):
                    yield name, s, l, half


def gelu_parts(h):
    sq = h * h
    th = jnp.tanh(GELU_C * (h + GELU_K * (h * sq)))
    return sq, th


def dot(a, b, ca, cb):
    return lax.dot_general(a, b, (((ca,), (cb,)), ((), ())), preferred_element_type=F32)


def step_kernel(*refs):
    it = iter(refs)
    take = lambda n: [next(it) for i in range(n)]
    x_saved, grad_out, x_next, w_up, w_down = take(5)
    acc, mast, mom1, mom2 = [dict(zip('ud', take(2))) for i in range(4)]
    nmast, nmom1, nmom2 = [dict(zip('ud', take(2))) for i in STREAMS]
    y_out, x_out, a_out, a_far, w_far = take(5)
    xr, tokr, pr = take(3)
    part, r1, r2o, r2f, r3, aw = [dict(zip('du', take(2))) for i in range(6)]
    gd, go, gx, ws = take(4)
    xv, yv, w1v, w2v, av, hv, fst, dwd, dwu = take(9)
    sb, so, r3v = [dict(zip('du', take(2))) for i in STREAMS]
    ssem, rsem, w1sem, w2sem, xsem, ysem, dwsem, sbsem, msem = take(9)

    me = lax.axis_index('fsdp')
    pos = {'z': lax.div(me, 8), 'y': bit(lax.div(me, 4)), 'x': bit(lax.div(me, 2))}
    core = bit(me)
    flip = {a: 1 - pos[a] for a in AXES}
    peer = {a: me + step * (1 - 2 * pos[a]) for a, step in (('z', 8), ('y', 4), ('x', 2))}
    peer['core'] = me + 1 - 2 * core
    spot = tuple(pos[a] for a in AXES)

    sem_ids = {}
    sends = {}

    def remote(key, src, dst, axis):
        n = sem_ids.setdefault(key, len(sem_ids))
        cp = pltpu.make_async_remote_copy(src_ref=src, dst_ref=dst, send_sem=ssem.at[n], recv_sem=rsem.at[n], device_id=(peer[axis],), device_id_type=MESH)
        cp.start()
        sends[key] = cp

    recv = lambda key: sends[key].wait_recv()
    unsent = set()

    def wait_send(key):
        if key in sends and key not in unsent:
            unsent.add(key)
            sends[key].wait_send()

    def cut(ref, i, fix, c0, n):
        return ref.at[(i,) + tuple(fix.get(a, slice(None)) for a in AXES) + (slice(None), pl.ds(c0, n))]

    def local(src, dst, sem):
        cp = pltpu.make_async_copy(src, dst, sem)
        cp.start()
        return cp

    loads = {'w1': [], 'w2': [], 'xa': [], 'xb': [], 'ya': [], 'yb': []}

    def ready(*names):
        for name in names:
            for cp in loads[name]:
                cp.wait()
            loads[name] = []

    def load_w1(s, l):
        loads['w1'] = [local(w_up.at[s, l, :, pl.ds(512 * c + 256 * core, 256)], w1v.at[:, pl.ds(256 * c, 256)], w1sem.at[c]) for c in range(8)]

    def load_w2(s, l):
        loads['w2'] = [local(w_down.at[s, l, c, core], w2v.at[pl.ds(256 * c, 256)], w2sem.at[c]) for c in range(8)]

    def load_new(kind, i):
        dst, sem, name, rows = (w1v, w1sem, 'w1', 128) if kind == 'u' else (w2v, w2sem, 'w2', 256)
        loads[name] = [local(aw[kind].at[i, c // 4, (c // 2) % 2, c % 2], dst.at[pl.ds(rows * c, rows)], sem.at[c]) for c in range(8)]

    def load_x(half, src):
        loads[('xa', 'xb')[half]] = [local(src, xv.at[pl.ds(T * half, T)], xsem.at[half])]

    def load_y(half, src):
        loads[('ya', 'yb')[half]] = [local(src, yv.at[pl.ds(T * half, T)], ysem.at[half])]

    def slab(n, size):
        return pl.ds(pl.multiple_of(n * size, size), size)

    def quad(g):
        return bit(flip['z'] + lax.div(g, 2)), bit(flip['y'] + g)

    def backward(i, g0, count, hook=None):
        def block(g, hook=None):
            zz, yy = quad(g)
            fs = slab(2 * zz + yy, TF)

            def body(n, carry):
                ts = slab(n, TM)
                h = dot(xv[ts, :], w1v[:, fs], 1, 0)
                da = dot(yv[ts, :], w2v[fs, :], 1, 1)
                sq, th = gelu_parts(h)
                cdf = 0.5 * (1.0 + th)
                av[ts, fs] = (h * cdf).astype(BF16)
                slope = cdf + 0.5 * h * (1.0 - th * th) * (GELU_C * (1.0 + 3.0 * GELU_K * sq))
                hv[ts, fs] = (da * slope).astype(BF16)
                return carry
            tiles = T // TM
            if hook is not None:
                lax.fori_loop(0, tiles, body, 0)
                hook()
                lax.fori_loop(tiles, 2 * tiles, body, 0)
            else:
                lax.fori_loop(0, 2 * tiles, body, 0)

            def out(n):
                return pltpu.make_async_copy(dwd.at[n], part['d'].at[i, zz, yy, n], dwsem.at[n])

            def body2(n, carry):
                f0 = slab(2 * (2 * zz + yy) + n, TM)

                def inner(c, carry):
                    cs = slab(c, TF)
                    dwd[n, :, cs] = dot(av[:, f0], yv[:, cs], 0, 0).astype(BF16)
                    return carry
                lax.fori_loop(0, D // TF, inner, 0)
                out(n).start()
                return carry
            lax.fori_loop(0, 2, body2, 0)
            for n in PAIR:
                out(n).wait()
        if count == 1:
            block(jnp.int32(g0), hook)
        else:
            def each(g, carry):
                block(g)
                return carry
            lax.fori_loop(g0, g0 + count, each, 0)

    def j3(i, half):
        def out(n):
            return pltpu.make_async_copy(dwu.at[n], part['u'].at[i, half, n], dwsem.at[n])

        def body(n, carry):
            def inner(c, carry):
                fs = slab(c, TF)
                res = dot(xv[:, slab(2 * half + n, TM)], hv[:, fs], 0, 0).astype(BF16)
                for e in PAIR:
                    dwu[n, e, :, fs] = res[128 * e:128 * e + 128]
                return carry
            lax.fori_loop(0, H // TF, inner, 0)
            out(n).start()
            return carry
        lax.fori_loop(0, 2, body, 0)
        for n in PAIR:
            out(n).wait()

    def proj(half, src, dst, w, cb, send=None):
        def body(n, carry):
            def inner(c, carry):
                cs = slab(c, TF)
                wt = w[cs, :] if cb else w[:, cs]
                fst[dst, slab(n, TM), cs] = dot(src[slab(T // TM * half + n, TM), :], wt, 1, cb)
                return carry
            return lax.fori_loop(0, D // TF, inner, carry)
        if send is None:
            lax.fori_loop(0, T // TM, body, 0)
            return
        for e in PAIR:
            lax.fori_loop(2 * e, 2 * e + 2, body, 0)
            rows = pl.ds(TF * e, TF)
            remote(('pr', send, e), fst.at[0, rows], pr.at[send, rows], 'core')

    def f1(half, many):
        def body(n, carry):
            ts = slab(T // TM * half + lax.div(n, H // TF), TM)
            fs = slab(lax.rem(n, H // TF), TF)
            h = dot(xv[ts, :], w1v[:, fs], 1, 0)
            sq, th = gelu_parts(h)
            av[ts, fs] = (h * (0.5 * (1.0 + th))).astype(BF16)
            return carry
        lax.fori_loop(0, many * (T // TM) * (H // TF), body, 0)

    def combine(n_pr, base):
        cps = []
        for e in PAIR:
            recv(('pr', n_pr, e))
            wait_send(('pr', n_pr, e))
            rows = pl.ds(TF * e, TF)
            cps.append(local(pr.at[n_pr, rows], fst.at[0, rows], msem.at[2 * e]))
        for e in PAIR:
            cps[e].wait()

            def body(n, carry):
                rows = slab(n, SUB)
                base[rows, :] = (base[rows, :].astype(F32) + (fst[1, rows, :] + fst[0, rows, :])).astype(BF16)
                return carry
            lax.fori_loop(TF * e // SUB, TF * (e + 1) // SUB, body, 0)

    def streams(kind, m):
        r = mat(*m[:2]) % len(ORDERS)
        return zip(STREAMS, COLS[kind], ORDERS[r:] + ORDERS[:r])

    last_so = {'d': None, 'u': None}
    last_gx = [None]
    first = {}

    def fetch(kind, items):
        cps = [local(src, dst, sbsem.at[n]) for n, (src, dst) in enumerate(items)]
        for cp in cps:
            cp.wait()

    def send_own(kind, m):
        i = mat(*m[:2])
        for q, (c0, n), (a, b, c) in streams(kind, m):
            fix = {a: pos[a], b: flip[b]}
            remote(('r2o', m, q), cut(part[kind], i, fix, c0, n), cut(r2o[kind], i, fix, c0, n), b)

    def send_half(kind, m, fix, which=AXES):
        i = mat(*m[:2])
        for q, (c0, n), (a, b, c) in streams(kind, m):
            if a in which:
                where = {**fix, a: flip[a]}
                key = ('r1', m, q)
                first.setdefault(key, []).append(key + (len(first.get(key, ())),))
                remote(first[key][-1], cut(part[kind], i, where, c0, n), cut(r1[kind], i, where, c0, n), a)

    def far_half(fix, q, c0, n):
        i = mat(*LAST[:2])
        part_of = lambda ref: ref.at[tuple(fix.get(a, slice(None)) for a in AXES) + (slice(None), pl.ds(c0, n))]
        key = ('far', q)
        first.setdefault(key, []).append(key + (len(first.get(key, ())),))
        remote(first[key][-1], cut(aw['d'], i, fix, c0, n), part_of(w_far), 'core')

    def service(m, step):
        s, l, kind = m
        i = mat(s, l)
        rows, wide = ROWS[kind], WIDE[kind]
        pa, a1, a2, a3, a4 = part[kind], r1[kind], r2o[kind], r2f[kind], r3[kind]
        key = lambda name, q: (name, m, q)
        if step == 1:
            for q, (c0, n), (a, b, c) in streams(kind, m):
                for k in first[key('r1', q)]:
                    recv(k)
                fix = {a: pos[a], b: flip[b]}
                remote(key('r2f', q), cut(a1, i, fix, c0, n), cut(a3, i, fix, c0, n), b)
        if step == 2:
            items = []
            for q, (c0, n), (a, b, c) in streams(kind, m):
                recv(key('r2o', q))
                recv(key('r2f', q))
                fix = {a: pos[a], b: pos[b], c: flip[c]}
                for e, src in enumerate((pa, a1, a2, a3)):
                    items.append((cut(src, i, fix, c0, n), sb[kind].at[e, :, pl.ds(c0, n)]))
            if last_so[kind] is not None:
                for q in STREAMS:
                    wait_send(('r3', last_so[kind], q))
            last_so[kind] = m
            fetch(kind, items)

            def body(n, carry):
                r = slab(n, SUB)
                v = sb[kind]
                so[kind][r, :] = (v[0, r, :].astype(F32) + v[1, r, :].astype(F32)) + (v[2, r, :].astype(F32) + v[3, r, :].astype(F32))
                return carry
            lax.fori_loop(0, rows // SUB, body, 0)
            for q, (c0, n), (a, b, c) in streams(kind, m):
                remote(key('r3', q), so[kind].at[:, pl.ds(c0, n)], a4.at[i, :, pl.ds(c0, n)], c)
        if step == 3:
            for q in STREAMS:
                recv(key('r3', q))
            if kind == 'u' and last_gx[0] is not None:
                wait_send(last_gx[0])
            items = [(src.at[(i,) + spot], sb[kind].at[e]) for e, src in enumerate((pa, a1, a2, a3))]
            fetch(kind, items + [(a4.at[i], r3v[kind])])

            def body(n, carry):
                r = slab(n, SUB)
                v = sb[kind]
                r3v[kind][r, :] = (v[0, r, :].astype(F32) + v[1, r, :].astype(F32)) + (v[2, r, :].astype(F32) + v[3, r, :].astype(F32)) + r3v[kind][r, :]
                return carry
            lax.fori_loop(0, rows // SUB, body, 0)
            if kind == 'd':
                local(r3v[kind], gd.at[i], msem.at[1]).wait()
                spec = pl.BlockSpec((64, D), lambda j: (j, 0))

                def body_d(g, ac, ma, m1, m2, oma, om1, om2, ow):
                    oma[...], om1[...], om2[...] = adam_update(ac[...], g[...], ma[...], m1[...], m2[...])
                    ow[...] = oma[...].astype(BF16)
                pltpu.emit_pipeline(body_d, grid=(4,), in_specs=[spec] * 5, out_specs=[spec] * 4)(
                    gd.at[i], acc['d'].at[s, l], mast['d'].at[s, l], mom1['d'].at[s, l], mom2['d'].at[s, l],
                    nmast['d'].at[s, l], nmom1['d'].at[s, l], nmom2['d'].at[s, l], aw['d'].at[(i,) + spot])
            else:
                last_gx[0] = ('gx', m)
                remote(('gx', m), r3v[kind].at[pl.ds(pl.multiple_of(64 * (1 - core), 64), 64)], gx.at[i], 'core')
                local(r3v[kind].at[pl.ds(pl.multiple_of(64 * core, 64), 64)], go.at[i], msem.at[1]).wait()
        if step == 4:
            recv(('gx', m))
            spec = pl.BlockSpec((64, 512), lambda j: (0, j))
            part_spec = pl.BlockSpec((64, 256), lambda j: (0, j))
            own_spec = pl.BlockSpec((64, 256), lambda j: (core, j))

            def body_u(g0, g1, ac, ma, m1, m2, oma, om1, om2, ow0, ow1):
                low = jnp.where(core == 0, g0[...], g1[...])
                high = jnp.where(core == 0, g1[...], g0[...])
                for h, g in ((0, low), (1, high)):
                    c = slice(256 * h, 256 * h + 256)
                    oma[:, c], om1[:, c], om2[:, c] = adam_update(ac[:, c], g, ma[:, c], m1[:, c], m2[:, c])
                wl, wh = oma[:, :256], oma[:, 256:]
                ow0[...] = jnp.where(core == 0, wl, wh).astype(BF16)
                ow1[...] = jnp.where(core == 0, wh, wl).astype(BF16)
            pltpu.emit_pipeline(body_u, grid=(8,), in_specs=[part_spec] * 2 + [spec] * 4, out_specs=[spec] * 3 + [own_spec, part_spec])(
                go.at[i], gx.at[i], acc['u'].at[s, l], mast['u'].at[s, l], mom1['u'].at[s, l], mom2['u'].at[s, l],
                nmast['u'].at[s, l], nmom1['u'].at[s, l], nmom2['u'].at[s, l], aw['u'].at[(i,) + spot], ws.at[i])
            remote(('ws', m), ws.at[i], aw['u'].at[(i,) + spot + (pl.ds(pl.multiple_of(64 * core, 64), 64),)], 'core')
        if step == 5:
            recv(('ws', m))
        w = aw[kind]
        if (kind == 'd' and step == 3) or step == 5:
            for q, (c0, n), (a, b, c) in streams(kind, m):
                v = cut(w, i, pos, c0, n)
                remote(key('a1', q), v, v, c)
        if step == 6:
            for q, (c0, n), (a, b, c) in streams(kind, m):
                recv(key('a1', q))
                v = cut(w, i, {a: pos[a], b: pos[b]}, c0, n)
                remote(key('a2', q), v, v, b)
        if step == 7:
            for q, (c0, n), (a, b, c) in streams(kind, m):
                recv(key('a2', q))
                v = cut(w, i, {a: pos[a]}, c0, n)
                remote(key('a3', q), v, v, a)
                if m == LAST:
                    far_half({a: pos[a]}, q, c0, n)

    load_x(0, x_saved.at[START + (0,)])
    load_w1(*START)
    load_y(0, grad_out.at[0, 0])
    load_w2(*START)
    barrier = pltpu.get_barrier_semaphore()
    for axis in ('x', 'y', 'z', 'core'):
        pl.semaphore_signal(barrier, inc=1, device_id=(peer[axis],), device_id_type=MESH)
    pl.semaphore_wait(barrier, 4)
    toks = [x_saved.at[0, 1, 0], grad_out.at[0, 0], x_saved.at[0, 0, 0], x_saved.at[1, 1, 0], grad_out.at[1, 0], x_saved.at[1, 0, 0], x_next.at[0, 0], x_next.at[1, 0]]
    xid = {(0, 1): 0, (0, 0): 2, (1, 1): 3, (1, 0): 5}
    for n, src in enumerate(toks):
        remote(('tok', n), src, (xv, yv)[n].at[pl.ds(T, T)] if n < 2 else xr.at[n], 'core')

    following = {(0, 1): (0, 0), (0, 0): (1, 1), (1, 1): (1, 0), (1, 0): None}
    jobs = jobs_of()
    steps = {m: iter(STEPS[m[2]]) for m in MATS.values()}
    for token in ''.join(ORDER):
        if token in MATS:
            service(MATS[token], next(steps[MATS[token]]))
            continue
        name, s, l, half = next(jobs)
        i = mat(s, l)
        nxt = following[s, l]
        own = pl.ds(0, T)
        if name == 'k':
            def arrive():
                for n in PAIR:
                    recv(('tok', n))
            m = (s, l, 'd')
            start = (s, l) == START
            if half == 0:
                ready('xa', 'ya', 'w1', 'w2')
                if l == 0:
                    recv(('tk', s))
                    load_y(1, tokr.at[s])
                if not start:
                    ready('xb', 'yb')
            g = half if start else 2 * half
            many = 2 if g == 2 or not start else 1
            backward(i, g, many, arrive if start and half == 0 else None)
            zz, yy = quad(jnp.int32(g))
            last = g + many == QUADS
            which = 'xy' if last else 'xyz' if half == 0 else 'xz'
            send_half('d', m, {'z': zz} if many == 2 else {'z': zz, 'y': yy}, which)
            if last:
                send_own('d', m)
                if nxt:
                    load_w2(*nxt)
                if l == 0 and nxt:
                    load_w1(*nxt)
                    wait_send(('tk', s))
                    load_y(0, grad_out.at[nxt[0], 0])
                    recv(('tok', 4))
                    load_y(1, xr.at[4])
        elif name == 'bk':
            proj(half, hv, 1 - half, w1v, 1, s if half else None)
            if half == 0:
                load_w1(*nxt)
        elif name == 'j3':
            j3(i, half)
            if half:
                send_half('u', (s, l, 'u'), {})
                send_own('u', (s, l, 'u'))
                n = xid[nxt] if nxt else 6
                load_x(0, x_saved.at[nxt[0], nxt[1], 0] if nxt else x_next.at[0, 0])
                recv(('tok', n))
                load_x(1, xr.at[n])
        elif name == 'cb':
            combine(s, yv)
            remote(('tk', s), yv.at[own], tokr.at[s], 'core')
        elif name == 'f1':
            if half == 0:
                for q in STREAMS:
                    recv(('a3', (s, l, 'u'), q))
                load_new('u', i)
                if l == 0:
                    ready('xa', 'xb')
                ready('w1')
            else:
                recv(('tk', 2 + s))
                load_x(1, tokr.at[2 + s])
                ready('xb')
            f1(half, 1 if l else 2)
            if (s, l) == LAST[:2]:
                if half:
                    remote('a_far', av.at[pl.ds(T, T)], a_far, 'core')
                else:
                    keep = [local(xv.at[own], x_out, msem.at[0]), local(av.at[own], a_out, msem.at[1])]
        elif name == 'f2' and (s, l) == LAST[:2]:
            for q, (c0, n), (a, b, c) in streams('d', LAST):
                recv(('a3', LAST, q))
                far_half({a: flip[a]}, q, c0, n)
            for cp in keep:
                cp.wait()
            for q in STREAMS:
                for k in first['far', q]:
                    recv(k)
            recv('a_far')
        elif name == 'f2':
            if half:
                for q in STREAMS:
                    recv(('a3', (s, l, 'd'), q))
                load_new('d', i)
                ready('w2')
            proj(half, av, 1 - half, w2v, 0, 2 + i if half else None)
        elif name == 'cf':
            if l:
                wait_send(('tk', 2 + s))
            combine(2 + i, xv)
            if l == 0:
                remote(('tk', 2 + s), xv.at[own], tokr.at[2 + s], 'core')
            else:
                local(xv.at[own], y_out, msem.at[2]).wait()
                load_x(0, x_next.at[1, 0])
                recv(('tok', 7))
                load_x(1, xr.at[7])
    for key in sends:
        wait_send(key)


def finish(*refs):
    states, (y0, x_in, a_in, a_far, w_far, aw), outs = refs[:6], refs[6:12], refs[12:19]
    stage_u, stage_d, yv, xv, av, wv, isem, osem, lsem = refs[19:]
    last = (LAYERS - 1,)
    loads = [(x_in, xv), (a_in, av.at[0]), (a_far, av.at[1])]
    for c in range(CHIPS):
        spot = (c // 4, c // 2 % 2, c % 2)
        for e, src in enumerate((aw.at[last + spot], w_far.at[spot])):
            loads.append((src, wv.at[e, pl.ds(256 * c, 256)]))
    loads = [pltpu.make_async_copy(src, dst, lsem.at[n]) for n, (src, dst) in enumerate(loads)]
    moves = [(y0, yv, outs[6].at[0, 0])]
    for n in range(6):
        buf = (stage_u, stage_d)[n % 2]
        for s in PAIR:
            for l in PAIR:
                slot = buf.at[n // 2, s, l]
                moves.append((states[n].at[s, l], slot, outs[n].at[s, l]))
    ins = [pltpu.make_async_copy(a, b, isem.at[n]) for n, (a, b, c) in enumerate(moves)]
    ends = [pltpu.make_async_copy(b, c, osem.at[n]) for n, (a, b, c) in enumerate(moves)]
    for cp in loads:
        cp.start()
    for cp in loads:
        cp.wait()
    for cp in ins:
        cp.start()
    def tile(n, carry):
        rows = pl.ds(n * TM, TM)

        def inner(c, carry):
            cs = pl.ds(pl.multiple_of(c * TM, TM), TM)
            mlp = dot(av[0, rows, :], wv[0, :, cs], 1, 0) + dot(av[1, rows, :], wv[1, :, cs], 1, 0)
            xv[rows, cs] = (xv[rows, cs].astype(F32) + mlp).astype(BF16)
            return carry
        return lax.fori_loop(0, D // TM, inner, carry)
    tiles = T // TM
    share = len(moves) // tiles
    for n in range(tiles):
        tile(n, 0)
        for k in range(share * n, len(moves) if n == tiles - 1 else share * n + share):
            ins[k].wait()
            ends[k].start()
    out = pltpu.make_async_copy(xv, outs[6].at[1, 0], lsem.at[0])
    out.start()
    for cp in ends + [out]:
        cp.wait()


def solution(mesh):
    tok_spec = P(None, 'fsdp')
    layer_spec = P(None, None, 'fsdp')
    rep_spec = P()

    def device_step(x_saved, grad_out, x_next, w_up, w_down, *state):
        def sds(shape, dtype=F32):
            return jax.ShapeDtypeStruct(shape, dtype)
        up, down = (2, 2, 64, 4096), (2, 2, 256, 1024)
        cube = (4, 2, 2, 2)
        pd, pu = cube + (256, D), cube + (128, H)
        states = [sds(up), sds(down)] * 3
        tok = sds((T, D), BF16)
        hid = sds((T, H), BF16)
        outs = states + [tok, tok, hid, hid, sds((2, 2, 2, 256, D), BF16)]
        n_main = len(outs)
        outs += [sds((CHIPS, T, D), BF16), sds((LAYERS, T, D), BF16), sds((6, T, D))]
        for i in range(4):
            outs += [sds(pd, BF16), sds(pu, BF16)]
        outs += [sds((4, 256, D)), sds((4, 128, H))]
        n_aw = len(outs)
        outs += [sds(pd, BF16), sds(pu, BF16)]
        outs += [sds((4, 256, D)), sds((4, 64, H)), sds((4, 64, H)), sds((4, 64, H), BF16)]
        any_spec = pl.BlockSpec(memory_space=pl.ANY)
        dma = pltpu.SemaphoreType.DMA
        tok_v, hid_v = pltpu.VMEM((2 * T, D), BF16), pltpu.VMEM((2 * T, H), BF16)
        sum_d, sum_u = pltpu.VMEM((256, D), F32), pltpu.VMEM((128, H), F32)
        pair_sem = dma((2,))
        scratch = [
            tok_v, tok_v, pltpu.VMEM((D, H), BF16), pltpu.VMEM((H, D), BF16),
            hid_v, hid_v, pltpu.VMEM((2, T, D), F32),
            pltpu.VMEM((2, 256, D), BF16), pltpu.VMEM((2, 2, 128, H), BF16),
            pltpu.VMEM((4, 256, D), BF16), pltpu.VMEM((4, 128, H), BF16),
            sum_d, sum_u, sum_d, sum_u,
            dma((SEMS,)), dma((SEMS,)), dma((CHIPS,)), dma((CHIPS,)), pair_sem, pair_sem, pair_sem, dma((12,)), dma((3,)),
        ]
        res = pl.pallas_call(
            step_kernel,
            out_shape=outs,
            in_specs=[any_spec] * (5 + len(state)),
            out_specs=[any_spec] * len(outs),
            scratch_shapes=scratch,
            compiler_params=pltpu.CompilerParams(collective_id=0, has_side_effects=True, vmem_limit_bytes=VMEM_CAP),
        )(x_saved, grad_out, x_next, w_up, w_down.reshape(2, 2, 8, 2, 256, D), *state)
        vm = pltpu.VMEM
        final = pl.pallas_call(
            finish,
            out_shape=states + [sds((2, 1, T, D), BF16)],
            in_specs=[any_spec] * 12,
            out_specs=[any_spec] * 7,
            scratch_shapes=[vm((3,) + up, F32), vm((3,) + down, F32), vm((T, D), BF16), vm((T, D), BF16), vm((2, T, H), BF16), vm((2, H, D), BF16), dma((32,)), dma((32,)), dma((32,))],
            compiler_params=pltpu.CompilerParams(vmem_limit_bytes=VMEM_CAP),
        )(*res[:n_main], res[n_aw])
        return tuple(final)

    return jax.shard_map(device_step, mesh=mesh, in_specs=(layer_spec, tok_spec, tok_spec, rep_spec, rep_spec) + (layer_spec,) * 8, out_specs=(layer_spec,) * 6 + (tok_spec,), check_vma=False)
```
